32 devices in a mesh: seq: 16 (over z, y, x), dp: 2 (over core).
Axes of the slice: x: 2, y: 2, z: 4, core: 2. Of those that a mesh axis runs over, the one named last changes fastest.
Arguments:
- block_pos: int32 [2, 32], P('dp'), may hold values from 0 to 31, as said below
- queries: bfloat16 [2, 2048, 2048], P('dp', 'seq'), may hold values from -8 to 8
- keys: bfloat16 [2, 2048, 2048], P('dp', 'seq'), may hold values from -4 to 4
- values: bfloat16 [2, 2048, 2048], P('dp', 'seq'), may hold values from -4 to 4
- attn_out: bfloat16 [2, 2048, 2048], P('dp', 'seq'), may hold values from -4 to 4, as said below
- log_sums: float32 [2, 16, 2048], P('dp', None, 'seq'), as said below
- grad_out: bfloat16 [2, 2048, 2048], P('dp', 'seq'), may hold values from -0.375 to 0.375
- out_weight: bfloat16 [2048, 2048], replicated, may hold values from -12 to 12
Outputs:
- grad_queries: bfloat16 [2, 2048, 2048], P('dp', 'seq')
- grad_keys: bfloat16 [2, 2048, 2048], P('dp', 'seq')
- grad_values: bfloat16 [2, 2048, 2048], P('dp', 'seq')
- grad_weight: float32 [2048, 2048], P('seq')
The draws below stay inside these ranges and needn't reach their ends.
Inputs may be any that keep to these rules, and one draw needn't show every extreme that they name: Each row is a permutation of 0 to 31; row block c (rows c * 64 to c * 64 + 63) holds the rows at positions block_pos[b, c] * 64 onward, in order. attn_out is the forward attention output: per head, exp(scores - log_sums) on the allowed keys times values, rounded to bfloat16. log_sums[b, h, t] is the log of the sum of exp(scores[b, h, t, u]) over the keys u with pos[b, u] <= pos[b, t].
All inputs are finite; a program needn't handle non-finite values.
Results may differ from the reference program's by a relative error of at most 0.0075.
Values may be sent and summed in bfloat16 or wider, within the bound.
A program may use at most 320 MiB of HBM per device.

```python
import jax
import jax.numpy as jnp
from jax import lax

HEADS = 16
HEAD_DIM = 128
DW = 2048
TOK_DEV = 128
HD = 2048
BLOCK = 64
GRID = 4
NC = 32
LEN = 2048
SEQS = 2
N_SEQ = 16


def fold_key(base, number):
    return jax.random.fold_in(base, number)


def saved_forward(key):
    base = fold_key(key, 11)
    tables = []
    for index in range(SEQS):
        tables.append(jax.random.permutation(fold_key(base, 100 + index), NC).astype(jnp.int32))
    table_all = jnp.stack(tables)
    width_all = HEADS * HEAD_DIM
    shape = (SEQS, LEN, width_all)
    query_raw = 2.0 * jax.random.truncated_normal(fold_key(base, 1), -4.0, 4.0, shape, jnp.float32)
    key_raw = jax.random.truncated_normal(fold_key(base, 2), -4.0, 4.0, shape, jnp.float32)
    value_raw = jax.random.truncated_normal(fold_key(base, 3), -4.0, 4.0, shape, jnp.float32)
    query_all = query_raw.astype(jnp.bfloat16).astype(jnp.float32)
    key_all = key_raw.astype(jnp.bfloat16).astype(jnp.float32)
    value_all = value_raw.astype(jnp.bfloat16).astype(jnp.float32)
    scaling = HEAD_DIM ** (-0.5)
    outputs = []
    logs = []
    for index in range(SEQS):
        row_index = jnp.arange(LEN, dtype=jnp.int32)
        positions = tables[index][row_index // BLOCK] * BLOCK + row_index % BLOCK
        allowed = positions[None, :] <= positions[:, None]

        def head_forward(pack):
            query_h, key_h, value_h = pack
            scores = jnp.dot(query_h, key_h.T, precision=lax.Precision.HIGHEST) * scaling
            scores = jnp.where(allowed, scores, -1e+30)
            row_max = jnp.max(scores, axis=1)
            log_row = row_max + jnp.log(jnp.sum(jnp.exp(scores - row_max[:, None]), axis=1))
            weights = jnp.exp(scores - log_row[:, None])
            return (jnp.dot(weights, value_h, precision=lax.Precision.HIGHEST), log_row)

        def to_heads(array):
            return jnp.transpose(array.reshape(LEN, HEADS, HEAD_DIM), (1, 0, 2))
        heads_out, heads_log = lax.map(head_forward, (to_heads(query_all[index]), to_heads(key_all[index]), to_heads(value_all[index])))
        outputs.append(jnp.transpose(heads_out, (1, 0, 2)).reshape(LEN, width_all))
        logs.append(heads_log)
    return (table_all, query_all, key_all, value_all, jnp.stack(outputs), jnp.stack(logs))


def draw_block_pos(key, part):
    return saved_forward(key)[0].astype(jnp.int32)


def draw_queries(key, part):
    return saved_forward(key)[1].astype(jnp.bfloat16)


def draw_keys(key, part):
    return saved_forward(key)[2].astype(jnp.bfloat16)


def draw_values(key, part):
    return saved_forward(key)[3].astype(jnp.bfloat16)


def draw_attn_out(key, part):
    return saved_forward(key)[4].astype(jnp.bfloat16)


def draw_log_sums(key, part):
    return saved_forward(key)[5].astype(jnp.float32)


def levels(key, dims, split, low, high):
    def one(axis_at, blocks):
        steps = jax.random.uniform(jax.random.fold_in(jax.random.fold_in(key, 6), axis_at), (blocks,), jnp.float32, low / len(split), high / len(split))
        return jnp.repeat(jnp.exp(steps), dims[axis_at] // blocks).reshape((-1,) + (1,) * (len(dims) - axis_at - 1))

    loudness = one(*split[0])
    for cut in split[1:]:
        loudness = loudness * one(*cut)
    return loudness


def scatter_about(own_key, dims, width, reach, cuts=(), kind=jnp.bfloat16):
    entries = width * jax.random.normal(own_key, dims, jnp.float32)
    if cuts:
        entries = entries * levels(own_key, dims, cuts, -0.22, 0.18)
    return jnp.clip(entries, -reach, reach).astype(kind)


def setup_inputs(seed: int = 0) -> dict:
    seeds = jax.random.split(jax.random.key(seed), 9)
    block_pos = draw_block_pos(jax.random.fold_in(seeds[8], 71), 0)
    queries = draw_queries(jax.random.fold_in(seeds[8], 71), 0)
    keys = draw_keys(jax.random.fold_in(seeds[8], 71), 0)
    values = draw_values(jax.random.fold_in(seeds[8], 71), 0)
    attn_out = draw_attn_out(jax.random.fold_in(seeds[8], 71), 0)
    log_sums = draw_log_sums(jax.random.fold_in(seeds[8], 71), 0)
    grad_out = scatter_about(seeds[6], (SEQS, LEN, DW), 0.0625, 0.375, ((0, 2), (1, 16)))
    out_weight = scatter_about(seeds[7], (HD, DW), 2.0, 12.0)
    return dict(block_pos=block_pos, queries=queries, keys=keys, values=values, attn_out=attn_out, log_sums=log_sums, grad_out=grad_out, out_weight=out_weight)


def run_tables():
    query_owner = jnp.arange(N_SEQ, dtype=jnp.int32)[:, None]
    key_owner = jnp.arange(N_SEQ, dtype=jnp.int32)[None, :]
    distance = (query_owner - key_owner) % N_SEQ
    query_run = (-distance) % GRID
    key_run = ((distance + query_run) // GRID) % GRID
    choose = jnp.arange(GRID, dtype=jnp.int32)
    query_onehot = (query_run[:, :, None] == choose[None, None, :]).astype(jnp.float32)
    key_onehot = (key_run[:, :, None] == choose[None, None, :]).astype(jnp.float32)
    return query_onehot, key_onehot


def grouped_sum(pairs, runs, pattern):
    grouped = jnp.einsum(pattern, pairs, runs, precision=lax.Precision.HIGHEST)
    rounded = lax.optimization_barrier(grouped.astype(jnp.bfloat16))
    return jnp.sum(rounded.astype(jnp.float32), axis=1)


def one_sequence(table_row, query_rows, key_rows, value_rows, saved_out, log_rows, cotangent, out_weight, query_onehot, key_onehot):
    length = query_rows.shape[0]
    width_all = query_rows.shape[1]
    head_count = log_rows.shape[0]
    head_dim = width_all // head_count
    scaling = head_dim ** -0.5
    grad_heads = jnp.dot(cotangent, out_weight.T, preferred_element_type=jnp.float32).astype(jnp.bfloat16)
    deltas = jnp.sum((grad_heads.astype(jnp.float32) * saved_out.astype(jnp.float32)).reshape(length, head_count, head_dim), axis=-1).T
    row_index = jnp.arange(length, dtype=jnp.int32)
    positions = table_row[row_index // BLOCK] * BLOCK + row_index % BLOCK
    allowed = positions[None, :] <= positions[:, None]

    def to_heads(array):
        return jnp.transpose(array.reshape(length, head_count, head_dim), (1, 0, 2))

    def per_head(pack):
        query_h, key_h, value_h, grad_h, log_h, delta_h = pack
        scores = jnp.dot(query_h, key_h.T, preferred_element_type=jnp.float32) * scaling
        attn_probs = jnp.where(allowed, jnp.exp(scores - log_h[:, None]), 0.0)
        probs_low = lax.optimization_barrier(attn_probs.astype(jnp.bfloat16))
        dprobs = jnp.dot(grad_h, value_h.T, preferred_element_type=jnp.float32)
        dscores = attn_probs * (dprobs - delta_h[:, None])
        dscores_low = lax.optimization_barrier(dscores.astype(jnp.bfloat16))
        probs_four = probs_low.astype(jnp.float32).reshape(N_SEQ, TOK_DEV, N_SEQ, TOK_DEV)
        dscore_four = dscores_low.astype(jnp.float32).reshape(N_SEQ, TOK_DEV, N_SEQ, TOK_DEV)
        query_four = query_h.astype(jnp.float32).reshape(N_SEQ, TOK_DEV, head_dim)
        key_four = key_h.astype(jnp.float32).reshape(N_SEQ, TOK_DEV, head_dim)
        grad_four = grad_h.astype(jnp.float32).reshape(N_SEQ, TOK_DEV, head_dim)
        value_pairs = jnp.einsum("iajb,iac->ijbc", probs_four, grad_four, precision=lax.Precision.HIGHEST)
        value_grad = grouped_sum(value_pairs, key_onehot, "ijbc,ijt->jtbc")
        key_pairs = scaling * jnp.einsum("iajb,iac->ijbc", dscore_four, query_four, precision=lax.Precision.HIGHEST)
        key_grad = grouped_sum(key_pairs, key_onehot, "ijbc,ijt->jtbc")
        query_pairs = scaling * jnp.einsum("iajb,jbc->ijac", dscore_four, key_four, precision=lax.Precision.HIGHEST)
        query_grad = grouped_sum(query_pairs, query_onehot, "ijac,ijt->itac")
        return (query_grad.reshape(length, head_dim), key_grad.reshape(length, head_dim), value_grad.reshape(length, head_dim))

    packed = (to_heads(query_rows), to_heads(key_rows), to_heads(value_rows), to_heads(grad_heads), log_rows, deltas)
    query_grad, key_grad, value_grad = lax.map(per_head, packed)

    def from_heads(array):
        return jnp.transpose(array, (1, 0, 2)).reshape(length, width_all).astype(jnp.bfloat16)

    weight_grad = jnp.dot(saved_out.T, cotangent, preferred_element_type=jnp.float32)
    return from_heads(query_grad), from_heads(key_grad), from_heads(value_grad), weight_grad


def reference(block_pos, queries, keys, values, attn_out, log_sums, grad_out, out_weight):
    query_onehot, key_onehot = run_tables()
    query_list = []
    key_list = []
    value_list = []
    weight_total = jnp.zeros(out_weight.shape, jnp.float32)
    for index in range(SEQS):
        outcome = one_sequence(block_pos[index], queries[index], keys[index], values[index], attn_out[index], log_sums[index], grad_out[index], out_weight, query_onehot, key_onehot)
        query_list.append(outcome[0])
        key_list.append(outcome[1])
        value_list.append(outcome[2])
        weight_total = weight_total + outcome[3]
    return (jnp.stack(query_list), jnp.stack(key_list), jnp.stack(value_list), weight_total)
```

```python
import functools

import jax
import jax.numpy as jnp
from jax import lax
from jax.experimental import pallas as pl
from jax.experimental.pallas import tpu as pltpu
from jax.sharding import PartitionSpec as P


def shifted(shard, axis, by):
    count = lax.axis_size(axis)
    return lax.ppermute(shard, axis, [(i, (i + by) % count) for i in range(count)])


def slot_positions(table_row, owners, half_rows):
    slot_ids = owners[:, None] * 2 + jnp.arange(2, dtype=jnp.int32)[None, :]
    pick_rows = (
        slot_ids[:, :, None] == jnp.arange(table_row.shape[0], dtype=jnp.int32)[None, None, :]
    ).astype(jnp.int32)
    block_ids = jnp.sum(pick_rows * table_row[None, None, :], axis=-1)
    offsets = jnp.arange(half_rows, dtype=jnp.int32)
    return (block_ids[:, :, None] * half_rows + offsets[None, None, :]).reshape(
        owners.shape[0], 2 * half_rows
    )


def block_core(
    query_rows, grad_rows, log_block, delta_block, key_rows, value_rows, allowed, scaling
):
    head_count = log_block.shape[0]
    query_len = query_rows.shape[0]
    key_len = key_rows.shape[0]
    query_heads = query_rows.reshape(query_len, head_count, -1)
    grad_split = grad_rows.reshape(query_len, head_count, -1)
    key_heads = key_rows.reshape(key_len, head_count, -1)
    value_heads = value_rows.reshape(key_len, head_count, -1)
    scores = (
        jnp.einsum("ahd,bhd->hab", query_heads, key_heads, preferred_element_type=jnp.float32)
        * scaling
    )
    attn_probs = jnp.where(allowed[None], jnp.exp(scores - log_block[:, :, None]), 0.0)
    probs_low = attn_probs.astype(jnp.bfloat16)
    dprobs = jnp.einsum("ahd,bhd->hab", grad_split, value_heads, preferred_element_type=jnp.float32)
    dscores = attn_probs * (dprobs - delta_block[:, :, None])
    dscores_low = dscores.astype(jnp.bfloat16)
    value_part = jnp.einsum(
        "hab,ahd->bhd", probs_low, grad_split, preferred_element_type=jnp.float32
    )
    key_part = (
        jnp.einsum("hab,ahd->bhd", dscores_low, query_heads, preferred_element_type=jnp.float32)
        * scaling
    )
    query_part = (
        jnp.einsum("hab,bhd->ahd", dscores_low, key_heads, preferred_element_type=jnp.float32)
        * scaling
    )
    return (
        query_part.reshape(query_len, -1),
        key_part.reshape(key_len, -1),
        value_part.reshape(key_len, -1),
    )


def block_grads(
    query_rows, grad_rows, log_block, delta_block, key_rows, value_rows, allowed, scaling
):
    parts = block_core(
        query_rows, grad_rows, log_block, delta_block, key_rows, value_rows, allowed, scaling
    )
    return (parts[0], parts[1].astype(jnp.bfloat16), parts[2].astype(jnp.bfloat16))


def grid_per_device(block_pos, queries, keys, values, attn_out, log_sums, grad_out, out_weight):
    dev_count = lax.axis_size("seq")
    grid_side = 4 + 4 * (dev_count // 64)
    my_index = lax.axis_index("seq")
    table_row = block_pos[0]
    own_queries = queries[0]
    tok_rows = own_queries.shape[0]
    half_rows = tok_rows // 2
    head_count = log_sums.shape[1]
    width_all = own_queries.shape[1]
    scaling = (width_all // head_count) ** (-0.5)
    cotangent = grad_out[0]
    grad_heads = lax.dot_general(
        cotangent, out_weight, (((1,), (1,)), ((), ())), preferred_element_type=jnp.float32
    ).astype(jnp.bfloat16)
    deltas = jnp.einsum(
        "ahd,ahd->ha",
        grad_heads.reshape(tok_rows, head_count, -1),
        attn_out[0].reshape(tok_rows, head_count, -1),
        preferred_element_type=jnp.float32,
    )
    query_pack = (own_queries[None], grad_heads[None], log_sums[0][None], deltas[None])
    key_pack = (keys[0][None], values[0][None])
    query_list = [query_pack]
    key_list = [key_pack]
    for offset in range(1, grid_side):
        query_list.append(
            (
                shifted(query_pack[0].astype(jnp.float32), "seq", offset).astype(jnp.bfloat16),
                shifted(query_pack[1].astype(jnp.float32), "seq", offset).astype(jnp.bfloat16),
                shifted(query_pack[2], "seq", offset),
                shifted(query_pack[3], "seq", offset),
            )
        )
        key_list.append(shifted((key_pack[0], key_pack[1]), "seq", offset * grid_side))
    query_stack = tuple(
        (jnp.concatenate([parcel[member] for parcel in query_list], axis=0) for member in range(4))
    )
    key_stack = tuple(
        (jnp.concatenate([parcel[member] for parcel in key_list], axis=0) for member in range(2))
    )
    query_rows = query_stack[0].reshape(-1, width_all)
    grad_rows = query_stack[1].reshape(-1, width_all)
    log_block = jnp.transpose(query_stack[2], (1, 0, 2)).reshape(head_count, -1)
    delta_block = jnp.transpose(query_stack[3], (1, 0, 2)).reshape(head_count, -1)
    query_owners = (my_index - jnp.arange(grid_side, dtype=jnp.int32)) % dev_count
    key_owners = (my_index - jnp.arange(grid_side, dtype=jnp.int32) * grid_side) % dev_count
    query_pos = slot_positions(table_row, query_owners, half_rows).reshape(-1)
    key_pos = slot_positions(table_row, key_owners, half_rows)
    query_total = jnp.zeros((grid_side * tok_rows, width_all), jnp.float32)
    key_results = []
    for offset in range(grid_side):
        key_now = key_stack[0][offset]
        value_now = key_stack[1][offset]
        allowed = key_pos[offset][None, :] <= query_pos[:, None]
        results = block_grads(
            query_rows, grad_rows, log_block, delta_block, key_now, value_now, allowed, scaling
        )
        query_total = query_total + results[0]
        key_results.append((results[1], results[2]))
    query_parts = query_total.astype(jnp.bfloat16).reshape(grid_side, tok_rows, width_all)
    query_sum = query_parts[0].astype(jnp.float32)
    for offset in range(1, grid_side):
        query_sum = query_sum + shifted(query_parts[offset], "seq", -offset).astype(jnp.float32)
    key_sum = key_results[0][0].astype(jnp.float32)
    value_sum = key_results[0][1].astype(jnp.float32)
    for offset in range(1, grid_side):
        returned = shifted(
            (key_results[offset][0], key_results[offset][1]), "seq", -offset * grid_side
        )
        key_sum = key_sum + returned[0].astype(jnp.float32)
        value_sum = value_sum + returned[1].astype(jnp.float32)
    columns = attn_out[0]
    weight_share = lax.psum_scatter(
        lax.dot_general(
            columns, cotangent, (((0,), (0,)), ((), ())), preferred_element_type=jnp.float32
        ),
        ("seq", "dp"),
        scatter_dimension=0,
        tiled=True,
    )
    weight_share = lax.all_gather(
        weight_share.astype(jnp.bfloat16), "dp", axis=0, tiled=True
    ).astype(weight_share.dtype)
    return (
        query_sum.astype(jnp.bfloat16)[None],
        key_sum.astype(jnp.bfloat16)[None],
        value_sum.astype(jnp.bfloat16)[None],
        weight_share,
    )


MESH = pl.DeviceIdType.MESH
ANY = pl.BlockSpec(memory_space=pl.ANY)


def enter(count, side, cores, me, core):
    barrier = pltpu.get_barrier_semaphore()
    plane = me // side * side
    for step in range(1, count):
        pl.semaphore_signal(
            barrier, inc=1, device_id=(lax.rem(me + step, count), core), device_id_type=MESH
        )
    total = count - 1
    for turn in range(1, cores):
        for step in range(side):
            peer = (plane + step, lax.rem(core + turn, cores))
            pl.semaphore_signal(barrier, inc=1, device_id=peer, device_id_type=MESH)
            total += 1
    pl.semaphore_wait(barrier, total)


def gather_kernel(
    count, side, cores, dim,
    q_in, k_in, v_in, g_in, s_in, a_in, b_in,
    q_out, k_out, v_out, g_out, s_out, a_out, b_out,
    send, recv, plane_send, plane_recv, local,
):
    me = lax.axis_index("seq")
    core = lax.axis_index("dp")
    column = lax.rem(me, side)
    plane = me - column
    half = b_out.shape[2]
    enter(count, side, cores, me, core)

    def head_pieces(head, owner):
        cut = pl.ds(pl.multiple_of(head * dim, dim), dim)
        pairs = [
            (source.at[:, cut], target.at[owner])
            for source, target in ((q_in, q_out), (k_in, k_out), (v_in, v_out), (g_in, g_out))
        ]
        return pairs + [(s_in.at[head], s_out.at[owner])]

    def plane_pieces(to_column, to_core, slot):
        pairs = []
        for part in range(side):
            cut = pl.ds(pl.multiple_of((part * side + to_column) * dim, dim), dim)
            pairs.append((a_in.at[:, cut], a_out.at[slot, :, pl.ds(part * dim, dim)]))
        cut = pl.ds(pl.multiple_of(to_core * half, half), half)
        return pairs + [(b_in.at[:, cut], b_out.at[slot])]

    def head_copies(head, owner, out_index, in_index, device):
        return [
            pltpu.make_async_remote_copy(
                source, target, send.at[at, out_index], recv.at[at, in_index],
                device_id=device, device_id_type=MESH,
            )
            for at, (source, target) in enumerate(head_pieces(head, owner))
        ]

    def plane_copies(to_column, to_core, slot, out_index, in_index, device):
        return [
            pltpu.make_async_remote_copy(
                source, target, plane_send.at[at, out_index], plane_recv.at[at, in_index],
                device_id=device, device_id_type=MESH,
            )
            for at, (source, target) in enumerate(plane_pieces(to_column, to_core, slot))
        ]

    own_slot = column * cores + core
    owns = [
        pltpu.make_async_copy(source, target, local.at[at])
        for at, (source, target) in enumerate(
            head_pieces(me, me) + plane_pieces(column, core, own_slot)
        )
    ]
    members = side * cores

    def plane_peer(step):
        slot = lax.rem(own_slot + step, members)
        return slot, slot // cores, lax.rem(slot, cores)

    @pl.loop(1, count)
    def _(step):
        peer = lax.rem(me + step, count)
        for copy in head_copies(peer, me, step, me, (peer, core)):
            copy.start()

    for copy in owns:
        copy.start()

    @pl.loop(1, members)
    def _(step):
        slot, to_column, to_core = plane_peer(step)
        for copy in plane_copies(
            to_column, to_core, own_slot, step, own_slot, (plane + to_column, to_core)
        ):
            copy.start()

    for copy in owns:
        copy.wait()

    @pl.loop(1, count)
    def _(step):
        peer = lax.rem(me + step, count)
        for copy in head_copies(peer, me, step, me, (peer, core)):
            copy.wait_send()
        for copy in head_copies(me, peer, step, peer, (peer, core)):
            copy.wait_recv()

    @pl.loop(1, members)
    def _(step):
        slot, to_column, to_core = plane_peer(step)
        device = (plane + to_column, to_core)
        for copy in plane_copies(to_column, to_core, own_slot, step, own_slot, device):
            copy.wait_send()
        for copy in plane_copies(column, core, slot, step, slot, device):
            copy.wait_recv()


def return_kernel(
    count, side, cores, dim,
    q_in, k_in, v_in, w_in,
    q_out, k_out, v_out, w_out,
    send, recv, line_send, line_recv, local,
):
    me = lax.axis_index("seq")
    core = lax.axis_index("dp")
    row = me // side
    column = lax.rem(me, side)
    enter(count, side, 1, me, core)

    def pieces(owner, head):
        cut = pl.ds(pl.multiple_of(head * dim, dim), dim)
        return [
            (source.at[owner], target.at[:, cut])
            for source, target in ((q_in, q_out), (k_in, k_out), (v_in, v_out))
        ]

    def copies(owner, head, out_index, in_index, device):
        return [
            pltpu.make_async_remote_copy(
                source, target, send.at[at, out_index], recv.at[at, in_index],
                device_id=device, device_id_type=MESH,
            )
            for at, (source, target) in enumerate(pieces(owner, head))
        ]

    def line_copy(to_row, slot, out_index, in_index, device):
        return pltpu.make_async_remote_copy(
            w_in.at[to_row], w_out.at[slot], line_send.at[out_index], line_recv.at[in_index],
            device_id=device, device_id_type=MESH,
        )

    owns = [
        pltpu.make_async_copy(source, target, local.at[at])
        for at, (source, target) in enumerate(
            pieces(me, me) + [(w_in.at[row], w_out.at[row])]
        )
    ]

    for step in range(1, side):
        to_row = lax.rem(row + step, side)
        line_copy(to_row, row, step, row, (to_row * side + column, core)).start()

    @pl.loop(1, count)
    def _(step):
        peer = lax.rem(me + step, count)
        for copy in copies(peer, me, step, me, (peer, core)):
            copy.start()

    for copy in owns:
        copy.start()
    for copy in owns:
        copy.wait()

    for step in range(1, side):
        to_row = lax.rem(row + step, side)
        device = (to_row * side + column, core)
        line_copy(to_row, row, step, row, device).wait_send()
        line_copy(row, to_row, step, to_row, device).wait_recv()

    @pl.loop(1, count)
    def _(step):
        peer = lax.rem(me + step, count)
        for copy in copies(peer, me, step, me, (peer, core)):
            copy.wait_send()
        for copy in copies(me, peer, step, peer, (peer, core)):
            copy.wait_recv()


def head_kernel(
    tile, scaling, table, q_in, k_in, v_in, g_in, s_in, q_out, k_out, v_out,
    q_row, k_row, v_row, g_row, s_row, dq, dk, dv,
):
    blocks = table.shape[0]
    length, _ = q_in.shape
    half = length // blocks
    lanes = 2 * half
    side_of = lax.broadcasted_iota(jnp.int32, s_row.shape[1:], 1) // half
    for block in range(blocks):
        place = table[block]
        source = pl.ds(block * half, half)
        target = pl.ds(pl.multiple_of(place * half, half), half)
        for raw, ordered in ((q_in, q_row), (k_in, k_row), (v_in, v_row), (g_in, g_row)):
            ordered[target, :] = raw[source, :]
        stats = s_in[block // 2]
        turned = pltpu.roll(stats, half, 1)
        parity = place % 2
        chosen = jnp.where(parity == block % 2, stats, turned)
        s_row[place // 2] = jnp.where(side_of == parity, chosen, s_row[place // 2])
    tiles = length // tile
    per_tile = tile // lanes
    dq[...] = jnp.zeros_like(dq)

    def pair(i, j, diagonal, sums):
        key_cut = pl.ds(j * tile, tile)
        query_cut = pl.ds(pl.multiple_of(i * tile, tile), tile)
        k_tile, v_tile = k_row[key_cut, :], v_row[key_cut, :]
        q_tile, g_tile = q_row[query_cut, :], g_row[query_cut, :]
        log_line = jnp.concatenate(
            [s_row[i * per_tile + m, 0:1, :] for m in range(per_tile)], axis=1
        )
        delta_line = jnp.concatenate(
            [s_row[i * per_tile + m, 1:2, :] for m in range(per_tile)], axis=1
        )
        by_rows = (((1,), (1,)), ((), ()))
        scores = lax.dot_general(k_tile, q_tile, by_rows, preferred_element_type=jnp.float32)
        probs = jnp.exp(scores * scaling - log_line)
        if diagonal:
            key_at = lax.broadcasted_iota(jnp.int32, (tile, tile), 0)
            query_at = lax.broadcasted_iota(jnp.int32, (tile, tile), 1)
            probs = jnp.where(key_at <= query_at, probs, 0.0)
        dprobs = lax.dot_general(v_tile, g_tile, by_rows, preferred_element_type=jnp.float32)
        dscores = (probs * (dprobs - delta_line)).astype(jnp.bfloat16)
        dv_sum = sums[1] + jnp.dot(
            probs.astype(jnp.bfloat16), g_tile, preferred_element_type=jnp.float32
        )
        dk_sum = sums[0] + jnp.dot(dscores, q_tile, preferred_element_type=jnp.float32)
        dq[query_cut, :] += lax.dot_general(
            dscores, k_tile, (((0,), (0,)), ((), ())), preferred_element_type=jnp.float32
        )
        return dk_sum, dv_sum

    for j in range(tiles):
        zero = jnp.zeros((tile, dq.shape[1]), jnp.float32)
        sums = pair(j, j, True, (zero, zero))
        if j + 1 < tiles:
            sums = lax.fori_loop(
                j + 1, tiles, lambda i, carry: pair(i, j, False, carry), sums
            )
        dk[pl.ds(j * tile, tile), :] = sums[0]
        dv[pl.ds(j * tile, tile), :] = sums[1]
    for block in range(blocks):
        place = table[block]
        target = pl.ds(block * half, half)
        source = pl.ds(pl.multiple_of(place * half, half), half)
        q_out[target, :] = (dq[source, :] * scaling).astype(q_out.dtype)
        k_out[target, :] = (dk[source, :] * scaling).astype(k_out.dtype)
        v_out[target, :] = dv[source, :].astype(v_out.dtype)


def head_per_device(
    side, cores, block_pos, queries, keys, values, attn_out, log_sums, grad_out, out_weight
):
    count = lax.axis_size("seq")
    rows = queries.shape[1]
    width = queries.shape[2]
    heads = log_sums.shape[1]
    dim = width // heads
    scaling = dim ** (-0.5)
    out_width = grad_out.shape[2]
    share = out_width // cores
    length = count * rows
    low = jnp.bfloat16
    cotangent = grad_out[0]
    grad_heads = lax.dot_general(
        cotangent, out_weight, (((1,), (1,)), ((), ())), preferred_element_type=jnp.float32
    ).astype(low)
    deltas = jnp.einsum(
        "ahd,ahd->ha",
        grad_heads.reshape(rows, heads, dim),
        attn_out[0].reshape(rows, heads, dim),
        preferred_element_type=jnp.float32,
    )
    stats = jnp.stack([log_sums[0], deltas], axis=1)
    stats = jnp.pad(stats, ((0, 0), (0, 6), (0, 0)))
    shapes = [jax.ShapeDtypeStruct((count, rows, dim), low)] * 4 + [
        jax.ShapeDtypeStruct((count, 8, rows), jnp.float32),
        jax.ShapeDtypeStruct((side * cores, rows, side * dim), low),
        jax.ShapeDtypeStruct((side * cores, rows, share), low),
    ]
    dma = pltpu.SemaphoreType.DMA
    members = side * cores
    q_all, k_all, v_all, g_all, s_all, a_all, b_all = pl.pallas_call(
        functools.partial(gather_kernel, count, side, cores, dim),
        out_shape=shapes,
        in_specs=[ANY] * 7,
        out_specs=[ANY] * 7,
        scratch_shapes=[
            dma((5, count)), dma((5, count)),
            dma((side + 1, members)), dma((side + 1, members)), dma((side + 6,)),
        ],
        compiler_params=pltpu.CompilerParams(collective_id=0, has_side_effects=True),
    )(queries[0], keys[0], values[0], grad_heads, stats, attn_out[0], cotangent)
    partial = lax.dot_general(
        a_all.reshape(members * rows, side * dim),
        b_all.reshape(members * rows, share),
        (((0,), (0,)), ((), ())),
        preferred_element_type=jnp.float32,
    ).astype(low)
    tile = min(512, length)
    vmem = pl.BlockSpec(memory_space=pltpu.VMEM)
    wide = (length, dim)
    parts = pl.pallas_call(
        functools.partial(head_kernel, tile, scaling),
        out_shape=[jax.ShapeDtypeStruct(wide, low)] * 3,
        in_specs=[pl.BlockSpec(memory_space=pltpu.SMEM)] + [vmem] * 5,
        out_specs=[vmem] * 3,
        scratch_shapes=[pltpu.VMEM(wide, low)] * 4
        + [pltpu.VMEM((count, 8, rows), jnp.float32)]
        + [pltpu.VMEM(wide, jnp.float32)] * 3,
        compiler_params=pltpu.CompilerParams(vmem_limit_bytes=56 * 1024 * 1024),
    )(
        block_pos[0], q_all.reshape(wide), k_all.reshape(wide), v_all.reshape(wide),
        g_all.reshape(wide), s_all,
    )
    pieces = [part.reshape(count, rows, dim) for part in parts]
    grad_queries, grad_keys, grad_values, w_all = pl.pallas_call(
        functools.partial(return_kernel, count, side, cores, dim),
        out_shape=[jax.ShapeDtypeStruct((rows, width), low)] * 3
        + [jax.ShapeDtypeStruct((side, dim, share), low)],
        in_specs=[ANY] * 4,
        out_specs=[ANY] * 4,
        scratch_shapes=[
            dma((3, count)), dma((3, count)), dma((side,)), dma((side,)), dma((4,)),
        ],
        compiler_params=pltpu.CompilerParams(collective_id=1, has_side_effects=True),
    )(*pieces, partial.reshape(side, dim, share))
    weight_share = jnp.sum(w_all.astype(jnp.float32), axis=0).astype(low)
    weight_share = lax.all_gather(weight_share, "dp", axis=1, tiled=True).astype(jnp.float32)
    return grad_queries[None], grad_keys[None], grad_values[None], weight_share


def make_per_device(mesh):
    count = mesh.shape["seq"]
    cores = mesh.shape["dp"]
    side = int(round(count ** 0.5))

    def per_device(block_pos, queries, keys, values, attn_out, log_sums, grad_out, out_weight):
        heads = log_sums.shape[1]
        arguments = (
            block_pos, queries, keys, values, attn_out, log_sums, grad_out, out_weight
        )
        if heads == count and side * side == count:
            return head_per_device(side, cores, *arguments)
        return grid_per_device(*arguments)

    return per_device


def solution(mesh):
    in_specs = (
        P("dp", None),
        P("dp", "seq", None),
        P("dp", "seq", None),
        P("dp", "seq", None),
        P("dp", "seq", None),
        P("dp", None, "seq"),
        P("dp", "seq", None),
        P(),
    )
    out_specs = (P("dp", "seq", None), P("dp", "seq", None), P("dp", "seq", None), P("seq", None))
    return jax.shard_map(
        make_per_device(mesh), mesh=mesh, in_specs=in_specs, out_specs=out_specs, check_vma=False
    )
```

```python
import functools

import jax
import jax.numpy as jnp
from jax import lax
from jax.experimental import pallas as pl
from jax.experimental.pallas import tpu as pltpu
from jax.sharding import PartitionSpec as P


def shifted(shard, axis, by):
    count = lax.axis_size(axis)
    return lax.ppermute(shard, axis, [(i, (i + by) % count) for i in range(count)])


def slot_positions(table_row, owners, half_rows):
    slot_ids = owners[:, None] * 2 + jnp.arange(2, dtype=jnp.int32)[None, :]
    pick_rows = (
        slot_ids[:, :, None] == jnp.arange(table_row.shape[0], dtype=jnp.int32)[None, None, :]
    ).astype(jnp.int32)
    block_ids = jnp.sum(pick_rows * table_row[None, None, :], axis=-1)
    offsets = jnp.arange(half_rows, dtype=jnp.int32)
    return (block_ids[:, :, None] * half_rows + offsets[None, None, :]).reshape(
        owners.shape[0], 2 * half_rows
    )


def block_core(
    query_rows, grad_rows, log_block, delta_block, key_rows, value_rows, allowed, scaling
):
    head_count = log_block.shape[0]
    query_len = query_rows.shape[0]
    key_len = key_rows.shape[0]
    query_heads = query_rows.reshape(query_len, head_count, -1)
    grad_split = grad_rows.reshape(query_len, head_count, -1)
    key_heads = key_rows.reshape(key_len, head_count, -1)
    value_heads = value_rows.reshape(key_len, head_count, -1)
    scores = (
        jnp.einsum("ahd,bhd->hab", query_heads, key_heads, preferred_element_type=jnp.float32)
        * scaling
    )
    attn_probs = jnp.where(allowed[None], jnp.exp(scores - log_block[:, :, None]), 0.0)
    probs_low = attn_probs.astype(jnp.bfloat16)
    dprobs = jnp.einsum("ahd,bhd->hab", grad_split, value_heads, preferred_element_type=jnp.float32)
    dscores = attn_probs * (dprobs - delta_block[:, :, None])
    dscores_low = dscores.astype(jnp.bfloat16)
    value_part = jnp.einsum(
        "hab,ahd->bhd", probs_low, grad_split, preferred_element_type=jnp.float32
    )
    key_part = (
        jnp.einsum("hab,ahd->bhd", dscores_low, query_heads, preferred_element_type=jnp.float32)
        * scaling
    )
    query_part = (
        jnp.einsum("hab,bhd->ahd", dscores_low, key_heads, preferred_element_type=jnp.float32)
        * scaling
    )
    return (
        query_part.reshape(query_len, -1),
        key_part.reshape(key_len, -1),
        value_part.reshape(key_len, -1),
    )


def block_grads(
    query_rows, grad_rows, log_block, delta_block, key_rows, value_rows, allowed, scaling
):
    parts = block_core(
        query_rows, grad_rows, log_block, delta_block, key_rows, value_rows, allowed, scaling
    )
    return (parts[0], parts[1].astype(jnp.bfloat16), parts[2].astype(jnp.bfloat16))


def grid_per_device(block_pos, queries, keys, values, attn_out, log_sums, grad_out, out_weight):
    dev_count = lax.axis_size("seq")
    grid_side = 4 + 4 * (dev_count // 64)
    my_index = lax.axis_index("seq")
    table_row = block_pos[0]
    own_queries = queries[0]
    tok_rows = own_queries.shape[0]
    half_rows = tok_rows // 2
    head_count = log_sums.shape[1]
    width_all = own_queries.shape[1]
    scaling = (width_all // head_count) ** (-0.5)
    cotangent = grad_out[0]
    grad_heads = lax.dot_general(
        cotangent, out_weight, (((1,), (1,)), ((), ())), preferred_element_type=jnp.float32
    ).astype(jnp.bfloat16)
    deltas = jnp.einsum(
        "ahd,ahd->ha",
        grad_heads.reshape(tok_rows, head_count, -1),
        attn_out[0].reshape(tok_rows, head_count, -1),
        preferred_element_type=jnp.float32,
    )
    query_pack = (own_queries[None], grad_heads[None], log_sums[0][None], deltas[None])
    key_pack = (keys[0][None], values[0][None])
    query_list = [query_pack]
    key_list = [key_pack]
    for offset in range(1, grid_side):
        query_list.append(
            (
                shifted(query_pack[0].astype(jnp.float32), "seq", offset).astype(jnp.bfloat16),
                shifted(query_pack[1].astype(jnp.float32), "seq", offset).astype(jnp.bfloat16),
                shifted(query_pack[2], "seq", offset),
                shifted(query_pack[3], "seq", offset),
            )
        )
        key_list.append(shifted((key_pack[0], key_pack[1]), "seq", offset * grid_side))
    query_stack = tuple(
        (jnp.concatenate([parcel[member] for parcel in query_list], axis=0) for member in range(4))
    )
    key_stack = tuple(
        (jnp.concatenate([parcel[member] for parcel in key_list], axis=0) for member in range(2))
    )
    query_rows = query_stack[0].reshape(-1, width_all)
    grad_rows = query_stack[1].reshape(-1, width_all)
    log_block = jnp.transpose(query_stack[2], (1, 0, 2)).reshape(head_count, -1)
    delta_block = jnp.transpose(query_stack[3], (1, 0, 2)).reshape(head_count, -1)
    query_owners = (my_index - jnp.arange(grid_side, dtype=jnp.int32)) % dev_count
    key_owners = (my_index - jnp.arange(grid_side, dtype=jnp.int32) * grid_side) % dev_count
    query_pos = slot_positions(table_row, query_owners, half_rows).reshape(-1)
    key_pos = slot_positions(table_row, key_owners, half_rows)
    query_total = jnp.zeros((grid_side * tok_rows, width_all), jnp.float32)
    key_results = []
    for offset in range(grid_side):
        key_now = key_stack[0][offset]
        value_now = key_stack[1][offset]
        allowed = key_pos[offset][None, :] <= query_pos[:, None]
        results = block_grads(
            query_rows, grad_rows, log_block, delta_block, key_now, value_now, allowed, scaling
        )
        query_total = query_total + results[0]
        key_results.append((results[1], results[2]))
    query_parts = query_total.astype(jnp.bfloat16).reshape(grid_side, tok_rows, width_all)
    query_sum = query_parts[0].astype(jnp.float32)
    for offset in range(1, grid_side):
        query_sum = query_sum + shifted(query_parts[offset], "seq", -offset).astype(jnp.float32)
    key_sum = key_results[0][0].astype(jnp.float32)
    value_sum = key_results[0][1].astype(jnp.float32)
    for offset in range(1, grid_side):
        returned = shifted(
            (key_results[offset][0], key_results[offset][1]), "seq", -offset * grid_side
        )
        key_sum = key_sum + returned[0].astype(jnp.float32)
        value_sum = value_sum + returned[1].astype(jnp.float32)
    columns = attn_out[0]
    weight_share = lax.psum_scatter(
        lax.dot_general(
            columns, cotangent, (((0,), (0,)), ((), ())), preferred_element_type=jnp.float32
        ),
        ("seq", "dp"),
        scatter_dimension=0,
        tiled=True,
    )
    weight_share = lax.all_gather(
        weight_share.astype(jnp.bfloat16), "dp", axis=0, tiled=True
    ).astype(weight_share.dtype)
    return (
        query_sum.astype(jnp.bfloat16)[None],
        key_sum.astype(jnp.bfloat16)[None],
        value_sum.astype(jnp.bfloat16)[None],
        weight_share,
    )


MESH = pl.DeviceIdType.MESH
ANY = pl.BlockSpec(memory_space=pl.ANY)


def enter(count, side, cores, me, core):
    barrier = pltpu.get_barrier_semaphore()
    plane = me // side * side
    for step in range(1, count):
        pl.semaphore_signal(
            barrier, inc=1, device_id=(lax.rem(me + step, count), core), device_id_type=MESH
        )
    total = count - 1
    for turn in range(1, cores):
        for step in range(side):
            peer = (plane + step, lax.rem(core + turn, cores))
            pl.semaphore_signal(barrier, inc=1, device_id=peer, device_id_type=MESH)
            total += 1
    pl.semaphore_wait(barrier, total)


def fused_kernel(
    count, side, cores, dim, tile, scaling,
    places, q_in, k_in, v_in, a_in, b_in, l_in, w_in,
    q_out, k_out, v_out, w_out,
    q_all, k_all, v_all, g_all, s_all, a_all, b_all,
    a_own, b_own, l_own, w_own, g_own, s_own,
    q_row, k_row, v_row, g_row, s_row, dq, dk, dv,
    q_back, k_back, v_back, w_part, w_line, w_half,
    send, recv, plane_send, plane_recv, line_send, line_recv,
    back_send, back_recv, half_send, half_recv, local,
):
    me = lax.axis_index("seq")
    core = lax.axis_index("dp")
    column = lax.rem(me, side)
    plane = me - column
    row = me // side
    half = b_all.shape[2]
    members = side * cores
    own_slot = column * cores + core
    low = jnp.bfloat16

    loads = [
        pltpu.make_async_copy(source, target, local.at[at])
        for at, (source, target) in enumerate(
            [(b_in, b_own), (w_in, w_own), (a_in, a_own), (l_in, l_own)]
        )
    ]
    for copy in loads:
        copy.start()
    enter(count, side, cores, me, core)

    def head_cut(head):
        return pl.ds(pl.multiple_of(head * dim, dim), dim)

    rows = a_all.shape[1]

    def owner_blocks(owner):
        return pl.ds(owner * 2, 2)

    def remote(source, target, sender, receiver, device):
        return pltpu.make_async_remote_copy(
            source, target, sender, receiver, device_id=device, device_id_type=MESH
        )

    def row_pieces(head, owner):
        cut = head_cut(head)
        return [
            (q_in.at[:, :, cut], q_all.at[owner_blocks(owner)]),
            (k_in.at[:, :, cut], k_all.at[owner_blocks(owner)]),
            (v_in.at[:, :, cut], v_all.at[owner_blocks(owner)]),
        ]

    def grad_pieces(head, owner):
        return [
            (g_own.at[head], g_all.at[owner_blocks(owner)]),
            (s_own.at[head], s_all.at[owner_blocks(owner)]),
        ]

    def head_copies(pieces, base, out_index, in_index, device):
        return [
            remote(source, target, send.at[base + at, out_index], recv.at[base + at, in_index], device)
            for at, (source, target) in enumerate(pieces)
        ]

    def plane_pieces(to_column, to_core, slot):
        pairs = []
        for part in range(side):
            cut = head_cut(part * side + to_column)
            pairs.append((a_in.at[:, cut], a_all.at[slot, :, pl.ds(part * dim, dim)]))
        cut = pl.ds(pl.multiple_of(to_core * half, half), half)
        return pairs + [(b_in.at[:, cut], b_all.at[slot])]

    def plane_copies(to_column, to_core, slot, out_index, in_index, device):
        return [
            remote(source, target, plane_send.at[at, out_index], plane_recv.at[at, in_index], device)
            for at, (source, target) in enumerate(plane_pieces(to_column, to_core, slot))
        ]

    def plane_peer(step):
        slot = lax.rem(own_slot + step, members)
        return slot, slot // cores, lax.rem(slot, cores)

    def line_copy(to_row, slot, out_index, in_index, device):
        return remote(
            w_part.at[to_row], w_line.at[slot], line_send.at[out_index],
            line_recv.at[in_index], device,
        )

    def back_pieces(owner, head):
        cut = head_cut(head)
        return [
            (source.at[owner], target.at[:, cut])
            for source, target in ((q_back, q_out), (k_back, k_out), (v_back, v_out))
        ]

    def back_copies(owner, head, out_index, in_index, device):
        return [
            remote(source, target, back_send.at[at, out_index], back_recv.at[at, in_index], device)
            for at, (source, target) in enumerate(back_pieces(owner, head))
        ]

    @pl.loop(1, count)
    def _(step):
        peer = lax.rem(me + step, count)
        for copy in head_copies(row_pieces(peer, me), 0, step, me, (peer, core)):
            copy.start()

    @pl.loop(1, members)
    def _(step):
        slot, to_column, to_core = plane_peer(step)
        for copy in plane_copies(
            to_column, to_core, own_slot, step, own_slot, (plane + to_column, to_core)
        ):
            copy.start()

    owns = [
        pltpu.make_async_copy(source, target, local.at[4 + at])
        for at, (source, target) in enumerate(
            row_pieces(me, me) + plane_pieces(column, core, own_slot)
        )
    ]
    for copy in owns:
        copy.start()
    for copy in loads:
        copy.wait()

    by_rows = (((1,), (1,)), ((), ()))
    by_columns = (((0,), (0,)), ((), ()))
    stat_rows = s_own.shape[2:]
    block_rows = rows // 2
    stat_at = lax.broadcasted_iota(jnp.int32, stat_rows, 0)
    early_half = lax.broadcasted_iota(jnp.int32, stat_rows, 1) < block_rows
    log_row = stat_at < 1

    @pl.loop(1, count + 1)
    def _(step):
        head = lax.rem(me + step, count)
        grads = lax.dot_general(
            b_own[...], w_own[head_cut(head), :], by_rows, preferred_element_type=jnp.float32
        ).astype(low)
        g_own[head] = grads.reshape(2, block_rows, dim)
        product = grads.astype(jnp.float32) * a_own[:, head_cut(head)].astype(jnp.float32)
        deltas = lax.dot_general(
            jnp.ones((stat_rows[0], dim), jnp.float32), product, by_rows,
            precision=lax.Precision.HIGHEST, preferred_element_type=jnp.float32,
        )
        logs = jnp.broadcast_to(l_own[pl.ds(head, 1), :], stat_rows)
        stats = jnp.where(log_row, logs, deltas)
        turned = pltpu.roll(stats, block_rows, 1)
        s_own[head, 0] = jnp.where(early_half, stats, turned)
        s_own[head, 1] = jnp.where(early_half, turned, stats)

        @pl.when(step > 1)
        def _():
            before = lax.rem(me + step - 1, count)
            for copy in head_copies(grad_pieces(before, me), 3, step - 1, me, (before, core)):
                copy.start()

    g_all[owner_blocks(me)] = g_own[me]
    s_all[owner_blocks(me)] = s_own[me]

    for copy in owns:
        copy.wait()

    @pl.loop(1, members)
    def _(step):
        slot, to_column, to_core = plane_peer(step)
        device = (plane + to_column, to_core)
        for copy in plane_copies(to_column, to_core, own_slot, step, own_slot, device):
            copy.wait_send()
        for copy in plane_copies(column, core, slot, step, slot, device):
            copy.wait_recv()

    rows_all = members * a_all.shape[1]
    grads_in = b_all[...].reshape(rows_all, half)
    for part in range(side):
        saved = a_all[:, :, pl.ds(part * dim, dim)].reshape(rows_all, dim)
        w_part[part] = lax.dot_general(
            saved, grads_in, by_columns, preferred_element_type=jnp.float32
        ).astype(low)
    w_line[row] = w_part[row]
    for step in range(1, side):
        to_row = lax.rem(row + step, side)
        line_copy(to_row, row, step, row, (to_row * side + column, core)).start()

    @pl.loop(1, count)
    def _(step):
        peer = lax.rem(me + step, count)
        device = (peer, core)
        for copy in head_copies(row_pieces(peer, me), 0, step, me, device):
            copy.wait_send()
        for copy in head_copies(grad_pieces(peer, me), 3, step, me, device):
            copy.wait_send()
        for copy in head_copies(row_pieces(me, peer), 0, step, peer, device):
            copy.wait_recv()
        for copy in head_copies(grad_pieces(me, peer), 3, step, peer, device):
            copy.wait_recv()

    blocks = places.shape[0] // 2
    length = count * rows
    for place in range(blocks):
        block = places[place]
        target = pl.ds(place * block_rows, block_rows)
        for raw, ordered in ((q_all, q_row), (k_all, k_row), (v_all, v_row), (g_all, g_row)):
            ordered[target, :] = raw[block]
    for pair_at in range(blocks // 2):
        early = s_all[places[2 * pair_at]]
        late = s_all[places[2 * pair_at + 1]]
        s_row[pair_at] = jnp.where(early_half, early, late)
    tiles = length // tile
    per_tile = tile // rows
    tile_blocks = tile // block_rows
    dq[...] = jnp.zeros_like(dq)

    def pair(i, j, diagonal, sums):
        key_cut = pl.ds(j * tile, tile)
        query_cut = pl.ds(pl.multiple_of(i * tile, tile), tile)
        k_tile, v_tile = k_row[key_cut, :], v_row[key_cut, :]
        q_tile, g_tile = q_row[query_cut, :], g_row[query_cut, :]
        log_line = jnp.concatenate(
            [s_row[i * per_tile + m, 0:1, :] for m in range(per_tile)], axis=1
        )
        delta_line = jnp.concatenate(
            [s_row[i * per_tile + m, 1:2, :] for m in range(per_tile)], axis=1
        )
        scores = lax.dot_general(k_tile, q_tile, by_rows, preferred_element_type=jnp.float32)
        probs = jnp.exp(scores * scaling - log_line)
        if diagonal:
            key_at = lax.broadcasted_iota(jnp.int32, (tile, tile), 0)
            query_at = lax.broadcasted_iota(jnp.int32, (tile, tile), 1)
            probs = jnp.where(key_at <= query_at, probs, 0.0)
        dprobs = lax.dot_general(v_tile, g_tile, by_rows, preferred_element_type=jnp.float32)
        dscores = (probs * (dprobs - delta_line)).astype(low)
        dv_sum = sums[1] + jnp.dot(
            probs.astype(low), g_tile, preferred_element_type=jnp.float32
        )
        dk_sum = sums[0] + jnp.dot(dscores, q_tile, preferred_element_type=jnp.float32)
        dq[pl.ds(i * tile_blocks, tile_blocks)] += lax.dot_general(
            dscores, k_tile, by_columns, preferred_element_type=jnp.float32
        ).reshape(tile_blocks, block_rows, dim)
        return dk_sum, dv_sum

    for j in range(tiles):
        zero = jnp.zeros((tile, dim), jnp.float32)
        sums = pair(j, j, True, (zero, zero))
        if j + 1 < tiles:
            sums = lax.fori_loop(
                j + 1, tiles, lambda i, carry: pair(i, j, False, carry), sums
            )
        key_blocks = pl.ds(j * tile_blocks, tile_blocks)
        dk[key_blocks] = sums[0].reshape(tile_blocks, block_rows, dim)
        dv[key_blocks] = sums[1].reshape(tile_blocks, block_rows, dim)
    for block in range(blocks):
        place = places[blocks + block]
        target = pl.ds(block % 2 * block_rows, block_rows)
        q_back[block // 2, target, :] = (dq[place] * scaling).astype(low)
        k_back[block // 2, target, :] = (dk[place] * scaling).astype(low)
        v_back[block // 2, target, :] = dv[place].astype(low)

    @pl.loop(1, count)
    def _(step):
        peer = lax.rem(me + step, count)
        for copy in back_copies(peer, me, step, me, (peer, core)):
            copy.start()

    returns = [
        pltpu.make_async_copy(source, target, local.at[at])
        for at, (source, target) in enumerate(back_pieces(me, me))
    ]
    for copy in returns:
        copy.start()

    for step in range(1, side):
        to_row = lax.rem(row + step, side)
        device = (to_row * side + column, core)
        line_copy(to_row, row, step, row, device).wait_send()
        line_copy(row, to_row, step, to_row, device).wait_recv()
    total = w_line[0].astype(jnp.float32)
    for part in range(1, side):
        total = total + w_line[part].astype(jnp.float32)
    w_half[core] = total.astype(low)

    def half_copy(slot, turn, other):
        return remote(
            w_half.at[slot], w_half.at[slot], half_send.at[turn], half_recv.at[slot], (me, other)
        )

    for turn in range(1, cores):
        half_copy(core, turn, lax.rem(core + turn, cores)).start()
    for turn in range(1, cores):
        other = lax.rem(core + turn, cores)
        half_copy(core, turn, other).wait_send()
        half_copy(other, turn, other).wait_recv()
    for slot in range(cores):
        w_out[:, pl.ds(slot * half, half)] = w_half[slot].astype(jnp.float32)

    for copy in returns:
        copy.wait()

    @pl.loop(1, count)
    def _(step):
        peer = lax.rem(me + step, count)
        for copy in back_copies(peer, me, step, me, (peer, core)):
            copy.wait_send()
        for copy in back_copies(me, peer, step, peer, (peer, core)):
            copy.wait_recv()


def head_per_device(
    side, cores, block_pos, queries, keys, values, attn_out, log_sums, grad_out, out_weight
):
    count = lax.axis_size("seq")
    rows = queries.shape[1]
    width = queries.shape[2]
    heads = log_sums.shape[1]
    dim = width // heads
    scaling = dim ** (-0.5)
    out_width = grad_out.shape[2]
    share = out_width // cores
    length = count * rows
    low = jnp.bfloat16
    table = block_pos[0]
    numbers = jnp.arange(table.shape[0], dtype=jnp.int32)
    inverse = jnp.sum(
        jnp.where(table[None, :] == numbers[:, None], numbers[None, :], 0), axis=1
    )
    block_rows = rows // 2
    places = jnp.concatenate([inverse, table])
    dma = pltpu.SemaphoreType.DMA
    members = side * cores
    tile = min(512, length)
    vmem = pl.BlockSpec(memory_space=pltpu.VMEM)
    wide = (length, dim)
    block_shape = (2 * count, block_rows, dim)
    split = (count, rows, dim)
    stat = (count, 8, rows)
    grad_queries, grad_keys, grad_values, weight_share = pl.pallas_call(
        functools.partial(fused_kernel, count, side, cores, dim, tile, scaling),
        out_shape=[jax.ShapeDtypeStruct((rows, width), low)] * 3
        + [jax.ShapeDtypeStruct((dim, out_width), jnp.float32)],
        in_specs=[pl.BlockSpec(memory_space=pltpu.SMEM)] + [ANY] * 7,
        out_specs=[ANY] * 3 + [vmem],
        scratch_shapes=[pltpu.VMEM(block_shape, low)] * 4
        + [
            pltpu.VMEM((2 * count, 8, rows), jnp.float32),
            pltpu.VMEM((members, rows, side * dim), low),
            pltpu.VMEM((members, rows, share), low),
            pltpu.VMEM((rows, width), low),
            pltpu.VMEM((rows, out_width), low),
            pltpu.VMEM((heads, rows), jnp.float32),
            pltpu.VMEM(out_weight.shape, low),
            pltpu.VMEM((count, 2, block_rows, dim), low),
            pltpu.VMEM((count, 2, 8, rows), jnp.float32),
        ]
        + [pltpu.VMEM(wide, low)] * 4
        + [pltpu.VMEM(stat, jnp.float32)]
        + [pltpu.VMEM(block_shape, jnp.float32)] * 3
        + [pltpu.VMEM(split, low)] * 3
        + [pltpu.VMEM((side, dim, share), low)] * 2
        + [pltpu.VMEM((cores, dim, share), low)]
        + [
            dma((5, count)), dma((5, count)),
            dma((side + 1, members)), dma((side + 1, members)),
            dma((side,)), dma((side,)),
            dma((3, count)), dma((3, count)),
            dma((cores,)), dma((cores,)), dma((side + 8,)),
        ],
        compiler_params=pltpu.CompilerParams(
            collective_id=0, has_side_effects=True, vmem_limit_bytes=60 * 1024 * 1024
        ),
    )(
        places,
        *(part.reshape(2, block_rows, width) for part in (queries, keys, values)),
        attn_out[0], grad_out[0], log_sums[0],
        out_weight,
    )
    return grad_queries[None], grad_keys[None], grad_values[None], weight_share


def make_per_device(mesh):
    count = mesh.shape["seq"]
    cores = mesh.shape["dp"]
    side = int(round(count ** 0.5))

    def per_device(block_pos, queries, keys, values, attn_out, log_sums, grad_out, out_weight):
        heads = log_sums.shape[1]
        arguments = (
            block_pos, queries, keys, values, attn_out, log_sums, grad_out, out_weight
        )
        if heads == count and side * side == count:
            return head_per_device(side, cores, *arguments)
        return grid_per_device(*arguments)

    return per_device


def solution(mesh):
    in_specs = (
        P("dp", None),
        P("dp", "seq", None),
        P("dp", "seq", None),
        P("dp", "seq", None),
        P("dp", "seq", None),
        P("dp", None, "seq"),
        P("dp", "seq", None),
        P(),
    )
    out_specs = (P("dp", "seq", None), P("dp", "seq", None), P("dp", "seq", None), P("seq", None))
    return jax.shard_map(
        make_per_device(mesh), mesh=mesh, in_specs=in_specs, out_specs=out_specs, check_vma=False
    )
```

```python
import functools

import jax
import jax.numpy as jnp
from jax import lax
from jax.experimental import pallas as pl
from jax.experimental.pallas import tpu as pltpu
from jax.sharding import PartitionSpec as P


def shifted(shard, axis, by):
    count = lax.axis_size(axis)
    return lax.ppermute(shard, axis, [(i, (i + by) % count) for i in range(count)])


def slot_positions(table_row, owners, half_rows):
    slot_ids = owners[:, None] * 2 + jnp.arange(2, dtype=jnp.int32)[None, :]
    pick_rows = (
        slot_ids[:, :, None] == jnp.arange(table_row.shape[0], dtype=jnp.int32)[None, None, :]
    ).astype(jnp.int32)
    block_ids = jnp.sum(pick_rows * table_row[None, None, :], axis=-1)
    offsets = jnp.arange(half_rows, dtype=jnp.int32)
    return (block_ids[:, :, None] * half_rows + offsets[None, None, :]).reshape(
        owners.shape[0], 2 * half_rows
    )


def block_core(
    query_rows, grad_rows, log_block, delta_block, key_rows, value_rows, allowed, scaling
):
    head_count = log_block.shape[0]
    query_len = query_rows.shape[0]
    key_len = key_rows.shape[0]
    query_heads = query_rows.reshape(query_len, head_count, -1)
    grad_split = grad_rows.reshape(query_len, head_count, -1)
    key_heads = key_rows.reshape(key_len, head_count, -1)
    value_heads = value_rows.reshape(key_len, head_count, -1)
    scores = (
        jnp.einsum("ahd,bhd->hab", query_heads, key_heads, preferred_element_type=jnp.float32)
        * scaling
    )
    attn_probs = jnp.where(allowed[None], jnp.exp(scores - log_block[:, :, None]), 0.0)
    probs_low = attn_probs.astype(jnp.bfloat16)
    dprobs = jnp.einsum("ahd,bhd->hab", grad_split, value_heads, preferred_element_type=jnp.float32)
    dscores = attn_probs * (dprobs - delta_block[:, :, None])
    dscores_low = dscores.astype(jnp.bfloat16)
    value_part = jnp.einsum(
        "hab,ahd->bhd", probs_low, grad_split, preferred_element_type=jnp.float32
    )
    key_part = (
        jnp.einsum("hab,ahd->bhd", dscores_low, query_heads, preferred_element_type=jnp.float32)
        * scaling
    )
    query_part = (
        jnp.einsum("hab,bhd->ahd", dscores_low, key_heads, preferred_element_type=jnp.float32)
        * scaling
    )
    return (
        query_part.reshape(query_len, -1),
        key_part.reshape(key_len, -1),
        value_part.reshape(key_len, -1),
    )


def block_grads(
    query_rows, grad_rows, log_block, delta_block, key_rows, value_rows, allowed, scaling
):
    parts = block_core(
        query_rows, grad_rows, log_block, delta_block, key_rows, value_rows, allowed, scaling
    )
    return (parts[0], parts[1].astype(jnp.bfloat16), parts[2].astype(jnp.bfloat16))


def grid_per_device(block_pos, queries, keys, values, attn_out, log_sums, grad_out, out_weight):
    dev_count = lax.axis_size("seq")
    grid_side = 4 + 4 * (dev_count // 64)
    my_index = lax.axis_index("seq")
    table_row = block_pos[0]
    own_queries = queries[0]
    tok_rows = own_queries.shape[0]
    half_rows = tok_rows // 2
    head_count = log_sums.shape[1]
    width_all = own_queries.shape[1]
    scaling = (width_all // head_count) ** (-0.5)
    cotangent = grad_out[0]
    grad_heads = lax.dot_general(
        cotangent, out_weight, (((1,), (1,)), ((), ())), preferred_element_type=jnp.float32
    ).astype(jnp.bfloat16)
    deltas = jnp.einsum(
        "ahd,ahd->ha",
        grad_heads.reshape(tok_rows, head_count, -1),
        attn_out[0].reshape(tok_rows, head_count, -1),
        preferred_element_type=jnp.float32,
    )
    query_pack = (own_queries[None], grad_heads[None], log_sums[0][None], deltas[None])
    key_pack = (keys[0][None], values[0][None])
    query_list = [query_pack]
    key_list = [key_pack]
    for offset in range(1, grid_side):
        query_list.append(
            (
                shifted(query_pack[0].astype(jnp.float32), "seq", offset).astype(jnp.bfloat16),
                shifted(query_pack[1].astype(jnp.float32), "seq", offset).astype(jnp.bfloat16),
                shifted(query_pack[2], "seq", offset),
                shifted(query_pack[3], "seq", offset),
            )
        )
        key_list.append(shifted((key_pack[0], key_pack[1]), "seq", offset * grid_side))
    query_stack = tuple(
        (jnp.concatenate([parcel[member] for parcel in query_list], axis=0) for member in range(4))
    )
    key_stack = tuple(
        (jnp.concatenate([parcel[member] for parcel in key_list], axis=0) for member in range(2))
    )
    query_rows = query_stack[0].reshape(-1, width_all)
    grad_rows = query_stack[1].reshape(-1, width_all)
    log_block = jnp.transpose(query_stack[2], (1, 0, 2)).reshape(head_count, -1)
    delta_block = jnp.transpose(query_stack[3], (1, 0, 2)).reshape(head_count, -1)
    query_owners = (my_index - jnp.arange(grid_side, dtype=jnp.int32)) % dev_count
    key_owners = (my_index - jnp.arange(grid_side, dtype=jnp.int32) * grid_side) % dev_count
    query_pos = slot_positions(table_row, query_owners, half_rows).reshape(-1)
    key_pos = slot_positions(table_row, key_owners, half_rows)
    query_total = jnp.zeros((grid_side * tok_rows, width_all), jnp.float32)
    key_results = []
    for offset in range(grid_side):
        key_now = key_stack[0][offset]
        value_now = key_stack[1][offset]
        allowed = key_pos[offset][None, :] <= query_pos[:, None]
        results = block_grads(
            query_rows, grad_rows, log_block, delta_block, key_now, value_now, allowed, scaling
        )
        query_total = query_total + results[0]
        key_results.append((results[1], results[2]))
    query_parts = query_total.astype(jnp.bfloat16).reshape(grid_side, tok_rows, width_all)
    query_sum = query_parts[0].astype(jnp.float32)
    for offset in range(1, grid_side):
        query_sum = query_sum + shifted(query_parts[offset], "seq", -offset).astype(jnp.float32)
    key_sum = key_results[0][0].astype(jnp.float32)
    value_sum = key_results[0][1].astype(jnp.float32)
    for offset in range(1, grid_side):
        returned = shifted(
            (key_results[offset][0], key_results[offset][1]), "seq", -offset * grid_side
        )
        key_sum = key_sum + returned[0].astype(jnp.float32)
        value_sum = value_sum + returned[1].astype(jnp.float32)
    columns = attn_out[0]
    weight_share = lax.psum_scatter(
        lax.dot_general(
            columns, cotangent, (((0,), (0,)), ((), ())), preferred_element_type=jnp.float32
        ),
        ("seq", "dp"),
        scatter_dimension=0,
        tiled=True,
    )
    weight_share = lax.all_gather(
        weight_share.astype(jnp.bfloat16), "dp", axis=0, tiled=True
    ).astype(weight_share.dtype)
    return (
        query_sum.astype(jnp.bfloat16)[None],
        key_sum.astype(jnp.bfloat16)[None],
        value_sum.astype(jnp.bfloat16)[None],
        weight_share,
    )


MESH = pl.DeviceIdType.MESH
ANY = pl.BlockSpec(memory_space=pl.ANY)


def enter(count, cores, me, core):
    barrier = pltpu.get_barrier_semaphore()
    for step in range(1, count):
        pl.semaphore_signal(
            barrier, inc=1, device_id=(lax.rem(me + step, count), core), device_id_type=MESH
        )
    total = count - 1
    for turn in range(1, cores):
        peer = (me, lax.rem(core + turn, cores))
        pl.semaphore_signal(barrier, inc=1, device_id=peer, device_id_type=MESH)
        total += 1
    pl.semaphore_wait(barrier, total)


def fused_kernel(
    count, side, cores, dim, tile, scaling,
    sources, places, q_in, k_in, v_in, a_in, b_in, l_in, w_in,
    q_out, k_out, v_out, w_out,
    q_all, k_all, v_all, g_all, s_all, a_all, b_all,
    a_own, b_own, l_own, w_own, g_own, s_own,
    q_row, k_row, v_row, g_row, s_row, dq, dk, dv,
    q_back, k_back, v_back, w_part, w_line, w_half, w_core, w_land,
    send, recv, plane_send, plane_recv, line_send, line_recv,
    back_send, back_recv, half_send, half_recv, core_send, core_recv, local,
):
    me = lax.axis_index("seq")
    core = lax.axis_index("dp")
    column = lax.rem(me, side)
    plane = me - column
    row = me // side
    half = w_half.shape[2]
    low = jnp.bfloat16

    loads = [
        pltpu.make_async_copy(source, target, local.at[at])
        for at, (source, target) in enumerate(
            [(b_in, b_own), (w_in, w_own), (a_in, a_own), (l_in, l_own)]
        )
    ]
    for copy in loads:
        copy.start()
    enter(count, cores, me, core)

    def head_cut(head):
        return pl.ds(pl.multiple_of(head * dim, dim), dim)

    rows = a_all.shape[1]

    def owner_blocks(owner):
        return pl.ds(owner * 2, 2)

    def remote(source, target, sender, receiver, device):
        return pltpu.make_async_remote_copy(
            source, target, sender, receiver, device_id=device, device_id_type=MESH
        )

    def row_pieces(head, owner):
        cut = head_cut(head)
        return [
            (q_in.at[:, :, cut], q_all.at[owner_blocks(owner)]),
            (k_in.at[:, :, cut], k_all.at[owner_blocks(owner)]),
            (v_in.at[:, :, cut], v_all.at[owner_blocks(owner)]),
        ]

    def grad_pieces(head, owner):
        return [
            (g_own.at[head], g_all.at[owner_blocks(owner)]),
            (s_own.at[head], s_all.at[owner_blocks(owner)]),
        ]

    def head_copies(pieces, base, out_index, in_index, device):
        return [
            remote(source, target, send.at[base + at, out_index], recv.at[base + at, in_index], device)
            for at, (source, target) in enumerate(pieces)
        ]

    def plane_pieces(to_column, slot):
        pairs = []
        for part in range(side):
            cut = head_cut(part * side + to_column)
            pairs.append((a_in.at[:, cut], a_all.at[slot, :, pl.ds(part * dim, dim)]))
        return pairs + [(b_in, b_all.at[slot])]

    def plane_copies(to_column, slot, out_index, in_index, device):
        return [
            remote(source, target, plane_send.at[at, out_index], plane_recv.at[at, in_index], device)
            for at, (source, target) in enumerate(plane_pieces(to_column, slot))
        ]

    def plane_peer(step):
        return lax.rem(column + step, side)

    def far_first(turn):
        far = count - side
        return jnp.where(turn < far, turn + side, lax.rem(turn - far + 1, side))

    def core_copy(to_core, slot, turn):
        return remote(
            w_core.at[to_core], w_land.at[slot], core_send.at[turn], core_recv.at[slot],
            (me, to_core),
        )

    def line_copy(to_row, slot, out_index, in_index, device):
        return remote(
            w_part.at[to_row], w_line.at[slot], line_send.at[out_index],
            line_recv.at[in_index], device,
        )

    def back_pieces(owner, head):
        cut = head_cut(head)
        return [
            (source.at[owner], target.at[:, cut])
            for source, target in ((q_back, q_out), (k_back, k_out), (v_back, v_out))
        ]

    def back_copies(owner, head, out_index, in_index, device):
        return [
            remote(source, target, back_send.at[at, out_index], back_recv.at[at, in_index], device)
            for at, (source, target) in enumerate(back_pieces(owner, head))
        ]

    @pl.loop(0, count - 1)
    def _(turn):
        step = far_first(turn)
        peer = lax.rem(me + step, count)
        for copy in head_copies(row_pieces(peer, me), 0, step, me, (peer, core)):
            copy.start()

    owns = [
        pltpu.make_async_copy(source, target, local.at[4 + at])
        for at, (source, target) in enumerate(
            row_pieces(me, me) + plane_pieces(column, column)
        )
    ]
    for copy in owns:
        copy.start()
    for copy in loads:
        copy.wait()

    by_rows = (((1,), (1,)), ((), ()))
    by_columns = (((0,), (0,)), ((), ()))
    stat_rows = s_own.shape[2:]
    block_rows = rows // 2
    stat_at = lax.broadcasted_iota(jnp.int32, stat_rows, 0)
    early_half = lax.broadcasted_iota(jnp.int32, stat_rows, 1) < block_rows
    log_row = stat_at < 1

    @pl.loop(0, count)
    def _(turn):
        head = lax.rem(me + far_first(turn), count)
        grads = lax.dot_general(
            b_own[...], w_own[head_cut(head), :], by_rows, preferred_element_type=jnp.float32
        ).astype(low)
        g_own[head] = grads.reshape(2, block_rows, dim)
        product = grads.astype(jnp.float32) * a_own[:, head_cut(head)].astype(jnp.float32)
        deltas = lax.dot_general(
            jnp.ones((stat_rows[0], dim), jnp.float32), product, by_rows,
            precision=lax.Precision.HIGHEST, preferred_element_type=jnp.float32,
        )
        logs = jnp.broadcast_to(l_own[pl.ds(head, 1), :], stat_rows)
        stats = jnp.where(log_row, logs, deltas)
        turned = pltpu.roll(stats, block_rows, 1)
        s_own[head, 0] = jnp.where(early_half, stats, turned)
        s_own[head, 1] = jnp.where(early_half, turned, stats)

        @pl.when(turn > 0)
        def _():
            step = far_first(turn - 1)
            before = lax.rem(me + step, count)
            for copy in head_copies(grad_pieces(before, me), 3, step, me, (before, core)):
                copy.start()

    for step in range(1, side):
        to_column = plane_peer(step)
        for copy in plane_copies(to_column, column, step, column, (plane + to_column, core)):
            copy.start()

    g_all[owner_blocks(me)] = g_own[me]
    s_all[owner_blocks(me)] = s_own[me]

    for copy in owns:
        copy.wait()

    for step in range(1, side):
        to_column = plane_peer(step)
        device = (plane + to_column, core)
        for copy in plane_copies(to_column, column, step, column, device):
            copy.wait_send()
        for copy in plane_copies(column, to_column, step, to_column, device):
            copy.wait_recv()

    rows_all = side * rows
    for to_core in range(cores):
        grads_in = b_all[:, :, pl.ds(to_core * half, half)].reshape(rows_all, half)
        for part in range(side):
            saved = a_all[:, :, pl.ds(part * dim, dim)].reshape(rows_all, dim)
            w_core[to_core, part] = lax.dot_general(
                saved, grads_in, by_columns, preferred_element_type=jnp.float32
            ).astype(low)
    for turn in range(1, cores):
        core_copy(lax.rem(core + turn, cores), core, turn).start()
    w_land[core] = w_core[core]
    for turn in range(1, cores):
        other = lax.rem(core + turn, cores)
        core_copy(other, core, turn).wait_send()
        core_copy(core, other, turn).wait_recv()
    for part in range(side):
        merged = w_land[0, part].astype(jnp.float32)
        for slot in range(1, cores):
            merged = merged + w_land[slot, part].astype(jnp.float32)
        w_part[part] = merged.astype(low)
    w_line[row] = w_part[row]
    for step in range(1, side):
        to_row = lax.rem(row + step, side)
        line_copy(to_row, row, step, row, (to_row * side + column, core)).start()

    @pl.loop(1, count)
    def _(step):
        peer = lax.rem(me + step, count)
        device = (peer, core)
        for copy in head_copies(row_pieces(peer, me), 0, step, me, device):
            copy.wait_send()
        for copy in head_copies(grad_pieces(peer, me), 3, step, me, device):
            copy.wait_send()
        for copy in head_copies(row_pieces(me, peer), 0, step, peer, device):
            copy.wait_recv()
        for copy in head_copies(grad_pieces(me, peer), 3, step, peer, device):
            copy.wait_recv()

    blocks = places.shape[0]
    length = count * rows
    for place in range(blocks):
        block = sources[place]
        target = pl.ds(place * block_rows, block_rows)
        for raw, ordered in ((q_all, q_row), (k_all, k_row), (v_all, v_row), (g_all, g_row)):
            ordered[target, :] = raw[block]
    for pair_at in range(blocks // 2):
        early = s_all[sources[2 * pair_at]]
        late = s_all[sources[2 * pair_at + 1]]
        s_row[pair_at] = jnp.where(early_half, early, late)
    tiles = length // tile
    per_tile = tile // rows
    tile_blocks = tile // block_rows
    dq[...] = jnp.zeros_like(dq)

    def pair(i, j, diagonal, sums):
        key_cut = pl.ds(j * tile, tile)
        query_cut = pl.ds(pl.multiple_of(i * tile, tile), tile)
        k_tile, v_tile = k_row[key_cut, :], v_row[key_cut, :]
        q_tile, g_tile = q_row[query_cut, :], g_row[query_cut, :]
        log_line = jnp.concatenate(
            [s_row[i * per_tile + m, 0:1, :] for m in range(per_tile)], axis=1
        )
        delta_line = jnp.concatenate(
            [s_row[i * per_tile + m, 1:2, :] for m in range(per_tile)], axis=1
        )
        scores = lax.dot_general(k_tile, q_tile, by_rows, preferred_element_type=jnp.float32)
        probs = jnp.exp(scores * scaling - log_line)
        if diagonal:
            key_at = lax.broadcasted_iota(jnp.int32, (tile, tile), 0)
            query_at = lax.broadcasted_iota(jnp.int32, (tile, tile), 1)
            probs = jnp.where(key_at <= query_at, probs, 0.0)
        dprobs = lax.dot_general(v_tile, g_tile, by_rows, preferred_element_type=jnp.float32)
        dscores = (probs * (dprobs - delta_line)).astype(low)
        dv_sum = sums[1] + jnp.dot(
            probs.astype(low), g_tile, preferred_element_type=jnp.float32
        )
        dk_sum = sums[0] + jnp.dot(dscores, q_tile, preferred_element_type=jnp.float32)
        dq[pl.ds(i * tile_blocks, tile_blocks)] += lax.dot_general(
            dscores, k_tile, by_columns, preferred_element_type=jnp.float32
        ).reshape(tile_blocks, block_rows, dim)
        return dk_sum, dv_sum

    for j in range(tiles):
        zero = jnp.zeros((tile, dim), jnp.float32)
        sums = pair(j, j, True, (zero, zero))
        if j + 1 < tiles:
            sums = lax.fori_loop(
                j + 1, tiles, lambda i, carry: pair(i, j, False, carry), sums
            )
        key_blocks = pl.ds(j * tile_blocks, tile_blocks)
        dk[key_blocks] = sums[0].reshape(tile_blocks, block_rows, dim)
        dv[key_blocks] = sums[1].reshape(tile_blocks, block_rows, dim)
    for block in range(blocks):
        place = places[block]
        target = pl.ds(block % 2 * block_rows, block_rows)
        q_back[block // 2, target, :] = (dq[place] * scaling).astype(low)
        k_back[block // 2, target, :] = (dk[place] * scaling).astype(low)
        v_back[block // 2, target, :] = dv[place].astype(low)

    @pl.loop(0, count - 1)
    def _(turn):
        step = far_first(turn)
        peer = lax.rem(me + step, count)
        for copy in back_copies(peer, me, step, me, (peer, core)):
            copy.start()

    returns = [
        pltpu.make_async_copy(source, target, local.at[at])
        for at, (source, target) in enumerate(back_pieces(me, me))
    ]
    for copy in returns:
        copy.start()

    for step in range(1, side):
        to_row = lax.rem(row + step, side)
        device = (to_row * side + column, core)
        line_copy(to_row, row, step, row, device).wait_send()
        line_copy(row, to_row, step, to_row, device).wait_recv()
    total = w_line[0].astype(jnp.float32)
    for part in range(1, side):
        total = total + w_line[part].astype(jnp.float32)
    w_half[core] = total.astype(low)

    def half_copy(slot, turn, other):
        return remote(
            w_half.at[slot], w_half.at[slot], half_send.at[turn], half_recv.at[slot], (me, other)
        )

    for turn in range(1, cores):
        half_copy(core, turn, lax.rem(core + turn, cores)).start()
    for turn in range(1, cores):
        other = lax.rem(core + turn, cores)
        half_copy(core, turn, other).wait_send()
        half_copy(other, turn, other).wait_recv()
    for slot in range(cores):
        w_out[:, pl.ds(slot * half, half)] = w_half[slot]

    for copy in returns:
        copy.wait()

    @pl.loop(1, count)
    def _(step):
        peer = lax.rem(me + step, count)
        for copy in back_copies(peer, me, step, me, (peer, core)):
            copy.wait_send()
        for copy in back_copies(me, peer, step, peer, (peer, core)):
            copy.wait_recv()


def head_per_device(
    side, cores, block_pos, queries, keys, values, attn_out, log_sums, grad_out, out_weight
):
    count = lax.axis_size("seq")
    rows = queries.shape[1]
    width = queries.shape[2]
    heads = log_sums.shape[1]
    dim = width // heads
    scaling = dim ** (-0.5)
    out_width = grad_out.shape[2]
    share = out_width // cores
    length = count * rows
    low = jnp.bfloat16
    table = block_pos[0]
    numbers = jnp.arange(table.shape[0], dtype=jnp.int32)
    inverse = jnp.sum(
        jnp.where(table[None, :] == numbers[:, None], numbers[None, :], 0), axis=1
    )
    block_rows = rows // 2
    dma = pltpu.SemaphoreType.DMA
    tile = min(512, length)
    vmem = pl.BlockSpec(memory_space=pltpu.VMEM)
    wide = (length, dim)
    block_shape = (2 * count, block_rows, dim)
    split = (count, rows, dim)
    stat = (count, 8, rows)
    grad_queries, grad_keys, grad_values, weight_share = pl.pallas_call(
        functools.partial(fused_kernel, count, side, cores, dim, tile, scaling),
        out_shape=[jax.ShapeDtypeStruct((rows, width), low)] * 3
        + [jax.ShapeDtypeStruct((dim, out_width), low)],
        in_specs=[pl.BlockSpec(memory_space=pltpu.SMEM)] * 2 + [ANY] * 7,
        out_specs=[ANY] * 3 + [vmem],
        scratch_shapes=[pltpu.VMEM(block_shape, low)] * 4
        + [
            pltpu.VMEM((2 * count, 8, rows), jnp.float32),
            pltpu.VMEM((side, rows, side * dim), low),
            pltpu.VMEM((side, rows, out_width), low),
            pltpu.VMEM((rows, width), low),
            pltpu.VMEM((rows, out_width), low),
            pltpu.VMEM((heads, rows), jnp.float32),
            pltpu.VMEM(out_weight.shape, low),
            pltpu.VMEM((count, 2, block_rows, dim), low),
            pltpu.VMEM((count, 2, 8, rows), jnp.float32),
        ]
        + [pltpu.VMEM(wide, low)] * 4
        + [pltpu.VMEM(stat, jnp.float32)]
        + [pltpu.VMEM(block_shape, jnp.float32)] * 3
        + [pltpu.VMEM(split, low)] * 3
        + [pltpu.VMEM((side, dim, share), low)] * 2
        + [pltpu.VMEM((cores, dim, share), low)]
        + [pltpu.VMEM((cores, side, dim, share), low)] * 2
        + [
            dma((5, count)), dma((5, count)),
            dma((side + 1, side)), dma((side + 1, side)),
            dma((side,)), dma((side,)),
            dma((3, count)), dma((3, count)),
            dma((cores,)), dma((cores,)), dma((cores,)), dma((cores,)), dma((side + 8,)),
        ],
        compiler_params=pltpu.CompilerParams(
            collective_id=0, has_side_effects=True, vmem_limit_bytes=60 * 1024 * 1024
        ),
    )(
        inverse, table,
        *(part.reshape(2, block_rows, width) for part in (queries, keys, values)),
        attn_out[0], grad_out[0], log_sums[0],
        out_weight,
    )
    grad_queries, grad_keys, grad_values, weight_share = pl.pallas_call(
        leave_kernel,
        out_shape=[jax.ShapeDtypeStruct((rows, width), low)] * 3
        + [jax.ShapeDtypeStruct((dim, out_width), jnp.float32)],
        in_specs=[vmem] * 4,
        out_specs=[vmem] * 4,
    )(grad_queries, grad_keys, grad_values, weight_share)
    return grad_queries[None], grad_keys[None], grad_values[None], weight_share


def leave_kernel(q_in, k_in, v_in, w_in, q_out, k_out, v_out, w_out):
    for source, target in ((q_in, q_out), (k_in, k_out), (v_in, v_out), (w_in, w_out)):
        target[...] = source[...].astype(target.dtype)


def make_per_device(mesh):
    count = mesh.shape["seq"]
    cores = mesh.shape["dp"]
    side = int(round(count ** 0.5))

    def per_device(block_pos, queries, keys, values, attn_out, log_sums, grad_out, out_weight):
        heads = log_sums.shape[1]
        arguments = (
            block_pos, queries, keys, values, attn_out, log_sums, grad_out, out_weight
        )
        if heads == count and side * side == count:
            return head_per_device(side, cores, *arguments)
        return grid_per_device(*arguments)

    return per_device


def solution(mesh):
    in_specs = (
        P("dp", None),
        P("dp", "seq", None),
        P("dp", "seq", None),
        P("dp", "seq", None),
        P("dp", "seq", None),
        P("dp", None, "seq"),
        P("dp", "seq", None),
        P(),
    )
    out_specs = (P("dp", "seq", None), P("dp", "seq", None), P("dp", "seq", None), P("seq", None))
    return jax.shard_map(
        make_per_device(mesh), mesh=mesh, in_specs=in_specs, out_specs=out_specs, check_vma=False
    )
```

```python
import functools

import jax
import jax.numpy as jnp
from jax import lax
from jax.experimental import pallas as pl
from jax.experimental.pallas import tpu as pltpu
from jax.sharding import PartitionSpec as P


def shifted(shard, axis, by):
    count = lax.axis_size(axis)
    return lax.ppermute(shard, axis, [(i, (i + by) % count) for i in range(count)])


def slot_positions(table_row, owners, half_rows):
    slot_ids = owners[:, None] * 2 + jnp.arange(2, dtype=jnp.int32)[None, :]
    pick_rows = (
        slot_ids[:, :, None] == jnp.arange(table_row.shape[0], dtype=jnp.int32)[None, None, :]
    ).astype(jnp.int32)
    block_ids = jnp.sum(pick_rows * table_row[None, None, :], axis=-1)
    offsets = jnp.arange(half_rows, dtype=jnp.int32)
    return (block_ids[:, :, None] * half_rows + offsets[None, None, :]).reshape(
        owners.shape[0], 2 * half_rows
    )


def block_core(
    query_rows, grad_rows, log_block, delta_block, key_rows, value_rows, allowed, scaling
):
    head_count = log_block.shape[0]
    query_len = query_rows.shape[0]
    key_len = key_rows.shape[0]
    query_heads = query_rows.reshape(query_len, head_count, -1)
    grad_split = grad_rows.reshape(query_len, head_count, -1)
    key_heads = key_rows.reshape(key_len, head_count, -1)
    value_heads = value_rows.reshape(key_len, head_count, -1)
    scores = (
        jnp.einsum("ahd,bhd->hab", query_heads, key_heads, preferred_element_type=jnp.float32)
        * scaling
    )
    attn_probs = jnp.where(allowed[None], jnp.exp(scores - log_block[:, :, None]), 0.0)
    probs_low = attn_probs.astype(jnp.bfloat16)
    dprobs = jnp.einsum("ahd,bhd->hab", grad_split, value_heads, preferred_element_type=jnp.float32)
    dscores = attn_probs * (dprobs - delta_block[:, :, None])
    dscores_low = dscores.astype(jnp.bfloat16)
    value_part = jnp.einsum(
        "hab,ahd->bhd", probs_low, grad_split, preferred_element_type=jnp.float32
    )
    key_part = (
        jnp.einsum("hab,ahd->bhd", dscores_low, query_heads, preferred_element_type=jnp.float32)
        * scaling
    )
    query_part = (
        jnp.einsum("hab,bhd->ahd", dscores_low, key_heads, preferred_element_type=jnp.float32)
        * scaling
    )
    return (
        query_part.reshape(query_len, -1),
        key_part.reshape(key_len, -1),
        value_part.reshape(key_len, -1),
    )


def block_grads(
    query_rows, grad_rows, log_block, delta_block, key_rows, value_rows, allowed, scaling
):
    parts = block_core(
        query_rows, grad_rows, log_block, delta_block, key_rows, value_rows, allowed, scaling
    )
    return (parts[0], parts[1].astype(jnp.bfloat16), parts[2].astype(jnp.bfloat16))


def grid_per_device(block_pos, queries, keys, values, attn_out, log_sums, grad_out, out_weight):
    dev_count = lax.axis_size("seq")
    grid_side = 4 + 4 * (dev_count // 64)
    my_index = lax.axis_index("seq")
    table_row = block_pos[0]
    own_queries = queries[0]
    tok_rows = own_queries.shape[0]
    half_rows = tok_rows // 2
    head_count = log_sums.shape[1]
    width_all = own_queries.shape[1]
    scaling = (width_all // head_count) ** (-0.5)
    cotangent = grad_out[0]
    grad_heads = lax.dot_general(
        cotangent, out_weight, (((1,), (1,)), ((), ())), preferred_element_type=jnp.float32
    ).astype(jnp.bfloat16)
    deltas = jnp.einsum(
        "ahd,ahd->ha",
        grad_heads.reshape(tok_rows, head_count, -1),
        attn_out[0].reshape(tok_rows, head_count, -1),
        preferred_element_type=jnp.float32,
    )
    query_pack = (own_queries[None], grad_heads[None], log_sums[0][None], deltas[None])
    key_pack = (keys[0][None], values[0][None])
    query_list = [query_pack]
    key_list = [key_pack]
    for offset in range(1, grid_side):
        query_list.append(
            (
                shifted(query_pack[0].astype(jnp.float32), "seq", offset).astype(jnp.bfloat16),
                shifted(query_pack[1].astype(jnp.float32), "seq", offset).astype(jnp.bfloat16),
                shifted(query_pack[2], "seq", offset),
                shifted(query_pack[3], "seq", offset),
            )
        )
        key_list.append(shifted((key_pack[0], key_pack[1]), "seq", offset * grid_side))
    query_stack = tuple(
        (jnp.concatenate([parcel[member] for parcel in query_list], axis=0) for member in range(4))
    )
    key_stack = tuple(
        (jnp.concatenate([parcel[member] for parcel in key_list], axis=0) for member in range(2))
    )
    query_rows = query_stack[0].reshape(-1, width_all)
    grad_rows = query_stack[1].reshape(-1, width_all)
    log_block = jnp.transpose(query_stack[2], (1, 0, 2)).reshape(head_count, -1)
    delta_block = jnp.transpose(query_stack[3], (1, 0, 2)).reshape(head_count, -1)
    query_owners = (my_index - jnp.arange(grid_side, dtype=jnp.int32)) % dev_count
    key_owners = (my_index - jnp.arange(grid_side, dtype=jnp.int32) * grid_side) % dev_count
    query_pos = slot_positions(table_row, query_owners, half_rows).reshape(-1)
    key_pos = slot_positions(table_row, key_owners, half_rows)
    query_total = jnp.zeros((grid_side * tok_rows, width_all), jnp.float32)
    key_results = []
    for offset in range(grid_side):
        key_now = key_stack[0][offset]
        value_now = key_stack[1][offset]
        allowed = key_pos[offset][None, :] <= query_pos[:, None]
        results = block_grads(
            query_rows, grad_rows, log_block, delta_block, key_now, value_now, allowed, scaling
        )
        query_total = query_total + results[0]
        key_results.append((results[1], results[2]))
    query_parts = query_total.astype(jnp.bfloat16).reshape(grid_side, tok_rows, width_all)
    query_sum = query_parts[0].astype(jnp.float32)
    for offset in range(1, grid_side):
        query_sum = query_sum + shifted(query_parts[offset], "seq", -offset).astype(jnp.float32)
    key_sum = key_results[0][0].astype(jnp.float32)
    value_sum = key_results[0][1].astype(jnp.float32)
    for offset in range(1, grid_side):
        returned = shifted(
            (key_results[offset][0], key_results[offset][1]), "seq", -offset * grid_side
        )
        key_sum = key_sum + returned[0].astype(jnp.float32)
        value_sum = value_sum + returned[1].astype(jnp.float32)
    columns = attn_out[0]
    weight_share = lax.psum_scatter(
        lax.dot_general(
            columns, cotangent, (((0,), (0,)), ((), ())), preferred_element_type=jnp.float32
        ),
        ("seq", "dp"),
        scatter_dimension=0,
        tiled=True,
    )
    weight_share = lax.all_gather(
        weight_share.astype(jnp.bfloat16), "dp", axis=0, tiled=True
    ).astype(weight_share.dtype)
    return (
        query_sum.astype(jnp.bfloat16)[None],
        key_sum.astype(jnp.bfloat16)[None],
        value_sum.astype(jnp.bfloat16)[None],
        weight_share,
    )


MESH = pl.DeviceIdType.MESH
ANY = pl.BlockSpec(memory_space=pl.ANY)


def enter(count, cores, me, core):
    barrier = pltpu.get_barrier_semaphore()
    for step in range(1, count):
        pl.semaphore_signal(
            barrier, inc=1, device_id=(lax.rem(me + step, count), core), device_id_type=MESH
        )
    total = count - 1
    for turn in range(1, cores):
        peer = (me, lax.rem(core + turn, cores))
        pl.semaphore_signal(barrier, inc=1, device_id=peer, device_id_type=MESH)
        total += 1
    pl.semaphore_wait(barrier, total)


def fused_kernel(
    count, side, cores, dim, tile, scaling,
    sources, places, q_in, k_in, v_in, a_in, b_in, l_in, w_in,
    q_out, k_out, v_out, w_out,
    q_all, k_all, v_all, g_all, s_all, a_all, b_all,
    a_own, b_own, l_own, w_own, g_own, s_own,
    q_row, k_row, v_row, g_row, s_row, dq, dk, dv,
    q_back, k_back, v_back, w_part, w_line, w_half, w_core, w_land,
    send, recv, plane_send, plane_recv, line_send, line_recv,
    back_send, back_recv, half_send, half_recv, core_send, core_recv, local,
):
    me = lax.axis_index("seq")
    core = lax.axis_index("dp")
    column = lax.rem(me, side)
    plane = me - column
    row = me // side
    half = w_half.shape[2]
    groups, _, _, _, sub = w_core.shape
    low = jnp.bfloat16

    loads = [
        pltpu.make_async_copy(source, target, local.at[at])
        for at, (source, target) in enumerate(
            [(b_in, b_own), (w_in, w_own), (a_in, a_own), (l_in, l_own)]
        )
    ]
    for copy in loads:
        copy.start()
    enter(count, cores, me, core)

    def head_cut(head):
        return pl.ds(pl.multiple_of(head * dim, dim), dim)

    rows = a_all.shape[1]

    def owner_blocks(owner):
        return pl.ds(owner * 2, 2)

    def remote(source, target, sender, receiver, device):
        return pltpu.make_async_remote_copy(
            source, target, sender, receiver, device_id=device, device_id_type=MESH
        )

    def row_pieces(head, owner):
        cut = head_cut(head)
        return [
            (q_in.at[:, :, cut], q_all.at[owner_blocks(owner)]),
            (k_in.at[:, :, cut], k_all.at[owner_blocks(owner)]),
            (v_in.at[:, :, cut], v_all.at[owner_blocks(owner)]),
        ]

    def grad_pieces(head, owner):
        return [
            (g_own.at[head], g_all.at[owner_blocks(owner)]),
            (s_own.at[head], s_all.at[owner_blocks(owner)]),
        ]

    def head_copies(pieces, base, out_index, in_index, device):
        return [
            remote(source, target, send.at[base + at, out_index], recv.at[base + at, in_index], device)
            for at, (source, target) in enumerate(pieces)
        ]

    def plane_pieces(to_column, slot):
        pairs = []
        for part in range(side):
            cut = head_cut(part * side + to_column)
            pairs.append((a_in.at[:, cut], a_all.at[slot, :, pl.ds(part * dim, dim)]))
        for group in range(groups):
            for to_core in range(cores):
                cut = pl.ds(to_core * half + group * sub, sub)
                pairs.append((b_in.at[:, cut], b_all.at[slot, :, cut]))
        return pairs

    def group_of(copies, group):
        first = side + group * cores if group else 0
        return copies[first : side + (group + 1) * cores]

    def plane_copies(to_column, slot, out_index, in_index, device):
        return [
            remote(source, target, plane_send.at[at, out_index], plane_recv.at[at, in_index], device)
            for at, (source, target) in enumerate(plane_pieces(to_column, slot))
        ]

    def plane_peer(step):
        return lax.rem(column + step, side)

    def far_first(turn):
        far = count - side
        return jnp.where(turn < far, turn + side, lax.rem(turn - far + 1, side))

    def core_copy(group, to_core, slot, turn):
        return remote(
            w_core.at[group, to_core], w_land.at[group, slot], core_send.at[group, turn],
            core_recv.at[group, slot], (me, to_core),
        )

    def line_copy(group, to_row, slot, out_index, in_index, device):
        return remote(
            w_part.at[group, to_row], w_line.at[group, slot], line_send.at[group, out_index],
            line_recv.at[group, in_index], device,
        )

    def back_pieces(owner, head):
        cut = head_cut(head)
        return [
            (source.at[owner], target.at[:, cut])
            for source, target in ((q_back, q_out), (k_back, k_out), (v_back, v_out))
        ]

    def back_copies(owner, head, out_index, in_index, device):
        return [
            remote(source, target, back_send.at[at, out_index], back_recv.at[at, in_index], device)
            for at, (source, target) in enumerate(back_pieces(owner, head))
        ]

    @pl.loop(0, count - 1)
    def _(turn):
        step = far_first(turn)
        peer = lax.rem(me + step, count)
        for copy in head_copies(row_pieces(peer, me), 0, step, me, (peer, core)):
            copy.start()

    owns = [
        pltpu.make_async_copy(source, target, local.at[4 + at])
        for at, (source, target) in enumerate(
            row_pieces(me, me) + plane_pieces(column, column)
        )
    ]
    for copy in owns:
        copy.start()
    for copy in loads:
        copy.wait()

    by_rows = (((1,), (1,)), ((), ()))
    by_columns = (((0,), (0,)), ((), ()))
    stat_rows = s_own.shape[2:]
    block_rows = rows // 2
    stat_at = lax.broadcasted_iota(jnp.int32, stat_rows, 0)
    early_half = lax.broadcasted_iota(jnp.int32, stat_rows, 1) < block_rows
    log_row = stat_at < 1

    @pl.loop(0, count)
    def _(turn):
        head = lax.rem(me + far_first(turn), count)
        grads = lax.dot_general(
            b_own[...], w_own[head_cut(head), :], by_rows, preferred_element_type=jnp.float32
        ).astype(low)
        g_own[head] = grads.reshape(2, block_rows, dim)
        product = grads.astype(jnp.float32) * a_own[:, head_cut(head)].astype(jnp.float32)
        deltas = lax.dot_general(
            jnp.ones((stat_rows[0], dim), jnp.float32), product, by_rows,
            precision=lax.Precision.HIGHEST, preferred_element_type=jnp.float32,
        )
        logs = jnp.broadcast_to(l_own[pl.ds(head, 1), :], stat_rows)
        stats = jnp.where(log_row, logs, deltas)
        turned = pltpu.roll(stats, block_rows, 1)
        s_own[head, 0] = jnp.where(early_half, stats, turned)
        s_own[head, 1] = jnp.where(early_half, turned, stats)

        @pl.when(turn > 0)
        def _():
            step = far_first(turn - 1)
            before = lax.rem(me + step, count)
            for copy in head_copies(grad_pieces(before, me), 3, step, me, (before, core)):
                copy.start()

    for group in range(groups):
        for step in range(1, side):
            to_column = plane_peer(step)
            device = (plane + to_column, core)
            for copy in group_of(
                plane_copies(to_column, column, step, column, device), group
            ):
                copy.start()

    g_all[owner_blocks(me)] = g_own[me]
    s_all[owner_blocks(me)] = s_own[me]

    for copy in owns:
        copy.wait()

    rows_all = side * rows

    def weight_part(part, grads_in):
        saved = a_all[:, :, pl.ds(part * dim, dim)].reshape(rows_all, dim)
        return lax.dot_general(
            saved, grads_in, by_columns, preferred_element_type=jnp.float32
        ).astype(low)

    def group_grads(to_core, group):
        cut = pl.ds(pl.multiple_of(to_core * half + group * sub, sub), sub)
        return b_all[:, :, cut].reshape(rows_all, sub)

    for group in range(groups):
        for step in range(1, side):
            to_column = plane_peer(step)
            device = (plane + to_column, core)
            for copy in group_of(
                plane_copies(column, to_column, step, to_column, device), group
            ):
                copy.wait_recv()
        for turn in range(1, cores):
            to_core = lax.rem(core + turn, cores)
            grads_in = group_grads(to_core, group)
            for part in range(side):
                w_core[group, to_core, part] = weight_part(part, grads_in)
            core_copy(group, to_core, core, turn).start()
        grads_in = group_grads(core, group)
        for part in range(side):
            w_land[group, core, part] = weight_part(part, grads_in)
        for turn in range(1, cores):
            other = lax.rem(core + turn, cores)
            core_copy(group, other, core, turn).wait_send()
            core_copy(group, core, other, turn).wait_recv()
        for part in range(side):
            merged = w_land[group, 0, part].astype(jnp.float32)
            for slot in range(1, cores):
                merged = merged + w_land[group, slot, part].astype(jnp.float32)
            w_part[group, part] = merged.astype(low)
        w_line[group, row] = w_part[group, row]
        for step in range(1, side):
            to_row = lax.rem(row + step, side)
            line_copy(
                group, to_row, row, step, row, (to_row * side + column, core)
            ).start()
    for step in range(1, side):
        to_column = plane_peer(step)
        device = (plane + to_column, core)
        for copy in plane_copies(to_column, column, step, column, device):
            copy.wait_send()

    @pl.loop(1, count)
    def _(step):
        peer = lax.rem(me + step, count)
        device = (peer, core)
        for copy in head_copies(row_pieces(peer, me), 0, step, me, device):
            copy.wait_send()
        for copy in head_copies(grad_pieces(peer, me), 3, step, me, device):
            copy.wait_send()
        for copy in head_copies(row_pieces(me, peer), 0, step, peer, device):
            copy.wait_recv()
        for copy in head_copies(grad_pieces(me, peer), 3, step, peer, device):
            copy.wait_recv()

    blocks = places.shape[0]
    length = count * rows
    for place in range(blocks):
        block = sources[place]
        target = pl.ds(place * block_rows, block_rows)
        for raw, ordered in ((q_all, q_row), (k_all, k_row), (v_all, v_row), (g_all, g_row)):
            ordered[target, :] = raw[block]
    for pair_at in range(blocks // 2):
        early = s_all[sources[2 * pair_at]]
        late = s_all[sources[2 * pair_at + 1]]
        s_row[pair_at] = jnp.where(early_half, early, late)
    tiles = length // tile
    per_tile = tile // rows
    tile_blocks = tile // block_rows
    dq[...] = jnp.zeros_like(dq)

    def pair(i, j, diagonal, sums):
        key_cut = pl.ds(j * tile, tile)
        query_cut = pl.ds(pl.multiple_of(i * tile, tile), tile)
        k_tile, v_tile = k_row[key_cut, :], v_row[key_cut, :]
        q_tile, g_tile = q_row[query_cut, :], g_row[query_cut, :]
        log_line = jnp.concatenate(
            [s_row[i * per_tile + m, 0:1, :] for m in range(per_tile)], axis=1
        )
        delta_line = jnp.concatenate(
            [s_row[i * per_tile + m, 1:2, :] for m in range(per_tile)], axis=1
        )
        scores = lax.dot_general(k_tile, q_tile, by_rows, preferred_element_type=jnp.float32)
        probs = jnp.exp(scores * scaling - log_line)
        if diagonal:
            key_at = lax.broadcasted_iota(jnp.int32, (tile, tile), 0)
            query_at = lax.broadcasted_iota(jnp.int32, (tile, tile), 1)
            probs = jnp.where(key_at <= query_at, probs, 0.0)
        dprobs = lax.dot_general(v_tile, g_tile, by_rows, preferred_element_type=jnp.float32)
        dscores = (probs * (dprobs - delta_line)).astype(low)
        dv_sum = sums[1] + jnp.dot(
            probs.astype(low), g_tile, preferred_element_type=jnp.float32
        )
        dk_sum = sums[0] + jnp.dot(dscores, q_tile, preferred_element_type=jnp.float32)
        dq[pl.ds(i * tile_blocks, tile_blocks)] += lax.dot_general(
            dscores, k_tile, by_columns, preferred_element_type=jnp.float32
        ).reshape(tile_blocks, block_rows, dim)
        return dk_sum, dv_sum

    for j in range(tiles):
        zero = jnp.zeros((tile, dim), jnp.float32)
        sums = pair(j, j, True, (zero, zero))
        if j + 1 < tiles:
            sums = lax.fori_loop(
                j + 1, tiles, lambda i, carry: pair(i, j, False, carry), sums
            )
        key_blocks = pl.ds(j * tile_blocks, tile_blocks)
        dk[key_blocks] = sums[0].reshape(tile_blocks, block_rows, dim)
        dv[key_blocks] = sums[1].reshape(tile_blocks, block_rows, dim)
    for block in range(blocks):
        place = places[block]
        target = pl.ds(block % 2 * block_rows, block_rows)
        q_back[block // 2, target, :] = (dq[place] * scaling).astype(low)
        k_back[block // 2, target, :] = (dk[place] * scaling).astype(low)
        v_back[block // 2, target, :] = dv[place].astype(low)

    @pl.loop(0, count - 1)
    def _(turn):
        step = far_first(turn)
        peer = lax.rem(me + step, count)
        for copy in back_copies(peer, me, step, me, (peer, core)):
            copy.start()

    returns = [
        pltpu.make_async_copy(source, target, local.at[at])
        for at, (source, target) in enumerate(back_pieces(me, me))
    ]
    for copy in returns:
        copy.start()

    for group in range(groups):
        for step in range(1, side):
            to_row = lax.rem(row + step, side)
            device = (to_row * side + column, core)
            line_copy(group, to_row, row, step, row, device).wait_send()
            line_copy(group, row, to_row, step, to_row, device).wait_recv()
        total = w_line[group, 0].astype(jnp.float32)
        for part in range(1, side):
            total = total + w_line[group, part].astype(jnp.float32)
        w_half[core, :, pl.ds(group * sub, sub)] = total.astype(low)

    def half_copy(slot, turn, other):
        return remote(
            w_half.at[slot], w_half.at[slot], half_send.at[turn], half_recv.at[slot], (me, other)
        )

    for turn in range(1, cores):
        half_copy(core, turn, lax.rem(core + turn, cores)).start()
    for turn in range(1, cores):
        other = lax.rem(core + turn, cores)
        half_copy(core, turn, other).wait_send()
        half_copy(other, turn, other).wait_recv()
    for slot in range(cores):
        w_out[:, pl.ds(slot * half, half)] = w_half[slot]

    for copy in returns:
        copy.wait()

    @pl.loop(1, count)
    def _(step):
        peer = lax.rem(me + step, count)
        for copy in back_copies(peer, me, step, me, (peer, core)):
            copy.wait_send()
        for copy in back_copies(me, peer, step, peer, (peer, core)):
            copy.wait_recv()


def head_per_device(
    side, cores, block_pos, queries, keys, values, attn_out, log_sums, grad_out, out_weight
):
    count = lax.axis_size("seq")
    rows = queries.shape[1]
    width = queries.shape[2]
    heads = log_sums.shape[1]
    dim = width // heads
    scaling = dim ** (-0.5)
    out_width = grad_out.shape[2]
    share = out_width // cores
    length = count * rows
    low = jnp.bfloat16
    table = block_pos[0]
    numbers = jnp.arange(table.shape[0], dtype=jnp.int32)
    inverse = jnp.sum(
        jnp.where(table[None, :] == numbers[:, None], numbers[None, :], 0), axis=1
    )
    block_rows = rows // 2
    groups = 2
    sub = share // groups
    pieces = side + groups * cores
    dma = pltpu.SemaphoreType.DMA
    tile = min(512, length)
    vmem = pl.BlockSpec(memory_space=pltpu.VMEM)
    wide = (length, dim)
    block_shape = (2 * count, block_rows, dim)
    split = (count, rows, dim)
    stat = (count, 8, rows)
    grad_queries, grad_keys, grad_values, weight_share = pl.pallas_call(
        functools.partial(fused_kernel, count, side, cores, dim, tile, scaling),
        out_shape=[jax.ShapeDtypeStruct((rows, width), low)] * 3
        + [jax.ShapeDtypeStruct((dim, out_width), low)],
        in_specs=[pl.BlockSpec(memory_space=pltpu.SMEM)] * 2 + [ANY] * 7,
        out_specs=[ANY] * 3 + [vmem],
        scratch_shapes=[pltpu.VMEM(block_shape, low)] * 4
        + [
            pltpu.VMEM((2 * count, 8, rows), jnp.float32),
            pltpu.VMEM((side, rows, side * dim), low),
            pltpu.VMEM((side, rows, out_width), low),
            pltpu.VMEM((rows, width), low),
            pltpu.VMEM((rows, out_width), low),
            pltpu.VMEM((heads, rows), jnp.float32),
            pltpu.VMEM(out_weight.shape, low),
            pltpu.VMEM((count, 2, block_rows, dim), low),
            pltpu.VMEM((count, 2, 8, rows), jnp.float32),
        ]
        + [pltpu.VMEM(wide, low)] * 4
        + [pltpu.VMEM(stat, jnp.float32)]
        + [pltpu.VMEM(block_shape, jnp.float32)] * 3
        + [pltpu.VMEM(split, low)] * 3
        + [pltpu.VMEM((groups, side, dim, sub), low)] * 2
        + [pltpu.VMEM((cores, dim, share), low)]
        + [pltpu.VMEM((groups, cores, side, dim, sub), low)] * 2
        + [
            dma((5, count)), dma((5, count)),
            dma((pieces, side)), dma((pieces, side)),
            dma((groups, side)), dma((groups, side)),
            dma((3, count)), dma((3, count)),
            dma((cores,)), dma((cores,)), dma((groups, cores)), dma((groups, cores)),
            dma((pieces + 7,)),
        ],
        compiler_params=pltpu.CompilerParams(
            collective_id=0, has_side_effects=True, vmem_limit_bytes=60 * 1024 * 1024
        ),
    )(
        inverse, table,
        *(part.reshape(2, block_rows, width) for part in (queries, keys, values)),
        attn_out[0], grad_out[0], log_sums[0],
        out_weight,
    )
    grad_queries, grad_keys, grad_values, weight_share = pl.pallas_call(
        leave_kernel,
        out_shape=[jax.ShapeDtypeStruct((rows, width), low)] * 3
        + [jax.ShapeDtypeStruct((dim, out_width), jnp.float32)],
        in_specs=[vmem] * 4,
        out_specs=[vmem] * 4,
    )(grad_queries, grad_keys, grad_values, weight_share)
    return grad_queries[None], grad_keys[None], grad_values[None], weight_share


def leave_kernel(q_in, k_in, v_in, w_in, q_out, k_out, v_out, w_out):
    for source, target in ((q_in, q_out), (k_in, k_out), (v_in, v_out), (w_in, w_out)):
        target[...] = source[...].astype(target.dtype)


def make_per_device(mesh):
    count = mesh.shape["seq"]
    cores = mesh.shape["dp"]
    side = int(round(count ** 0.5))

    def per_device(block_pos, queries, keys, values, attn_out, log_sums, grad_out, out_weight):
        heads = log_sums.shape[1]
        arguments = (
            block_pos, queries, keys, values, attn_out, log_sums, grad_out, out_weight
        )
        if heads == count and side * side == count:
            return head_per_device(side, cores, *arguments)
        return grid_per_device(*arguments)

    return per_device


def solution(mesh):
    in_specs = (
        P("dp", None),
        P("dp", "seq", None),
        P("dp", "seq", None),
        P("dp", "seq", None),
        P("dp", "seq", None),
        P("dp", None, "seq"),
        P("dp", "seq", None),
        P(),
    )
    out_specs = (P("dp", "seq", None), P("dp", "seq", None), P("dp", "seq", None), P("seq", None))
    return jax.shard_map(
        make_per_device(mesh), mesh=mesh, in_specs=in_specs, out_specs=out_specs, check_vma=False
    )
```
